128 devices in a mesh: row: 8 (over z, core), col: 16 (over x, y).
Axes of the slice: x: 4, y: 4, z: 4, core: 2. Of those that a mesh axis runs over, the one named last changes fastest.
Arguments:
- hamiltonian: bfloat16 [4096, 4096], P('row', 'col'), may hold values from -0.3 to 0.3
- pattern: int32 [32, 32], replicated, may hold values from 0 to 1, as said below
- tile_lists: int32 [128, 8], replicated, may hold values from 0 to 31, as said below
- orders: int32 [128], replicated, may hold values from 6 to 8
- shift: float32 [1], replicated, may hold values from -0.5 to 0.5
Outputs:
- density: bfloat16 [4096, 4096], P('row', 'col')
- php: float32 [4096, 4096], P('row', 'col')
The draws below stay inside these ranges and needn't reach their ends.
Inputs may be any that keep to these rules, and one draw needn't show every extreme that they name: `pattern`: Symmetric, with zeros on the diagonal. `tile_lists`: row s begins with tile s * 32 // 128; its entries lie in distinct groups of 2 consecutive tiles, and the second lies in the group that shares a group of 4 consecutive tiles with the first. Entries from position orders[s] on are not used.
All inputs are finite; a program needn't handle non-finite values.
Results may differ from the reference program's by a relative error of at most 0.0073.
Values may be sent and summed in bfloat16 or wider, within the bound.
No kernel may reach another device: no remote copies, remote signals or barrier semaphores. Data moves between devices by JAX's collectives and lax.ppermute only.
A program may use at most 64 MiB of HBM per device.

```python
import jax
import jax.numpy as jnp
from jax import lax

TILE = 128
TPC = 2
MAXT = 8
MINT = 6
ITERS = 3
NB = 32
NH = 4096
SUBS = 128
CW = 32


def draw_hamiltonian(key, part):
    raw = jax.random.truncated_normal(key, -4.0, 4.0, (NH, NH), jnp.float32) * 0.05
    mirrored = (raw + raw.T) * 0.5 ** 0.5
    return mirrored.astype(jnp.bfloat16)


def draw_pattern(key, part):
    picks = jax.random.randint(jax.random.fold_in(key, 5), (NB, NB), 0, 4, dtype=jnp.int32)
    upper = jnp.triu((picks == 0).astype(jnp.int32), 1)
    return (upper + upper.T).astype(jnp.int32)


def one_list(key, index):
    groups = NB // TPC
    center = index * CW // TILE
    home = center // TPC
    partner = jnp.bitwise_xor(home, 1)
    scores = jax.random.permutation(jax.random.fold_in(key, 7), groups).astype(jnp.int32)
    positions = jnp.arange(groups, dtype=jnp.int32)
    scores = jnp.where(positions == home, -2, scores)
    scores = jnp.where(positions == partner, -1, scores)
    chosen = jnp.argsort(scores, stable=True)[:MAXT].astype(jnp.int32)
    offsets = jax.random.randint(jax.random.fold_in(key, 11), (MAXT,), 0, TPC, dtype=jnp.int32)
    tiles = chosen * TPC + offsets
    return tiles.at[0].set(center.astype(jnp.int32))


def draw_tile_lists(key, part):
    keys = jax.random.split(jax.random.fold_in(key, 3), SUBS)
    return jax.vmap(one_list)(keys, jnp.arange(SUBS, dtype=jnp.int32)).astype(jnp.int32)


def with_ends(values, rng, smallest, top_value):
    longest = values.shape.index(max(values.shape))
    spots = []
    for shift in (0, 1):
        where = [jax.random.randint(jax.random.fold_in(rng, axis), (), 0, length) for axis, length in enumerate(values.shape)]
        where[longest] = (where[longest] + shift) % values.shape[longest]
        spots.append(tuple(where))
    return values.at[spots[0]].set(smallest).at[spots[1]].set(top_value)


def setup_inputs(seed: int = 0) -> dict:
    key_of = jax.random.split(jax.random.key(seed), 6)
    hamiltonian = draw_hamiltonian(jax.random.fold_in(key_of[5], 71), 0)
    pattern = draw_pattern(jax.random.fold_in(key_of[5], 71), 0)
    tile_lists = draw_tile_lists(jax.random.fold_in(key_of[5], 71), 0)
    orders = with_ends(jax.random.randint(key_of[3], (SUBS,), MINT, MAXT + 1), jax.random.fold_in(key_of[3], 1), MINT, MAXT).astype(jnp.int32)
    shift = jnp.clip(jax.random.uniform(key_of[4], (1,), jnp.float32, -0.5, 0.5), -0.5, 0.5)
    return {"hamiltonian": hamiltonian, "pattern": pattern, "tile_lists": tile_lists, "orders": orders, "shift": shift}


def masked_blocks(hamiltonian, pattern):
    count = pattern.shape[0]
    keep = jnp.maximum(pattern, jnp.eye(count, dtype=jnp.int32))
    blocks = hamiltonian.reshape(count, TILE, count, TILE).transpose(0, 2, 1, 3)
    return jnp.where(keep[:, :, None, None] > 0, blocks, jnp.zeros_like(blocks))

def newton_density(sub, live_rows, potential):
    eye = jnp.eye(sub.shape[0], dtype=jnp.float32)
    shifted = sub.astype(jnp.float32) - potential * eye * live_rows[None, :]
    row_squares = lax.optimization_barrier(jnp.sum(shifted * shifted, axis=1))
    scale = jnp.abs(potential) + 2.0 * jnp.sqrt(jnp.max(row_squares) + 1e-06)
    iterate = (shifted / scale).astype(jnp.bfloat16)
    product = shifted
    for step in range(ITERS):
        square = jnp.dot(iterate, iterate, preferred_element_type=jnp.float32)
        factor = (1.5 * eye - 0.5 * square).astype(jnp.bfloat16)
        product = jnp.dot(iterate, factor, preferred_element_type=jnp.float32)
        if step + 1 < ITERS:
            iterate = product.astype(jnp.bfloat16)
    return 0.5 * (eye - product)

def reference(hamiltonian, pattern, tile_lists, orders, shift):
    count = pattern.shape[0]
    blocks = masked_blocks(hamiltonian, pattern)
    potential = shift[0]
    total = tile_lists.shape[0]
    width = count * TILE // total

    def solve(index):
        tiles = tile_lists[index]
        live = jnp.arange(MAXT, dtype=jnp.int32) < orders[index]
        sub = jnp.take(jnp.take(blocks, tiles, axis=0), tiles, axis=1)
        both = live[:, None] & live[None, :]
        sub = jnp.where(both[:, :, None, None], sub, jnp.zeros_like(sub))
        sub = sub.transpose(0, 2, 1, 3).reshape(MAXT * TILE, MAXT * TILE)
        live_rows = jnp.repeat(live.astype(jnp.float32), TILE)
        dens = newton_density(sub, live_rows, potential)
        offset = (index * width % TILE).astype(jnp.int32)
        central = lax.dynamic_slice_in_dim(dens, offset, width, 1).astype(jnp.bfloat16)
        central = central.astype(jnp.float32).reshape(MAXT, TILE, width)
        chooser = ((tiles[:, None] == jnp.arange(count, dtype=jnp.int32)[None, :]) & live[:, None]).astype(jnp.float32)
        placed = jnp.einsum('ia,itw->atw', chooser, central)
        return placed.astype(jnp.bfloat16)
    pieces = lax.map(solve, jnp.arange(total, dtype=jnp.int32))
    density = pieces.transpose(1, 2, 0, 3).reshape(count * TILE, total * width)
    ham = blocks.transpose(0, 2, 1, 3).reshape(count * TILE, count * TILE)
    hp = jnp.dot(ham, density, preferred_element_type=jnp.float32).astype(jnp.bfloat16)
    php = jnp.dot(density, hp, preferred_element_type=jnp.float32)
    return (density, php)
```

```python
import jax
import jax.numpy as jnp
from jax import lax
from jax.experimental import pallas as pl
from jax.experimental.pallas import tpu as pltpu
from jax.sharding import PartitionSpec as P

TILE = 128
MAXT = 8
NB = 32
ROWS = 8
COLS = 16
SUBS = 128
CW = 32
N = MAXT * TILE
RT = NB // ROWS
CT = NB // COLS
F32 = jnp.float32
BF16 = jnp.bfloat16


def kept(pattern, a, b):
    return (pattern[a * NB + b] > 0) | (a == b)


def solve_kernel(ids, lists, orders, pattern, shift, gathered, panel, groups, raw, x, f, d, sems):
    s = ids[1] * ROWS + ids[0]
    order = orders[s]
    potential = shift[0]
    tiles = [lists[s * MAXT + i] for i in range(MAXT)]

    def copy(i, j):
        a, b = tiles[i], tiles[j]
        owner = a // RT * COLS + b // CT
        return pltpu.make_async_copy(
            gathered.at[owner, pl.ds(a % RT * TILE, TILE), pl.ds(b % CT * TILE, TILE)],
            raw.at[pl.ds(i * TILE, TILE), pl.ds(j * TILE, TILE)],
            sems.at[i, j],
        )

    for i in range(MAXT):
        for j in range(MAXT):
            copy(i, j).start()
    rows = lax.broadcasted_iota(jnp.int32, (TILE, TILE), 0)
    cols = lax.broadcasted_iota(jnp.int32, (TILE, TILE), 1)
    eye = jnp.where(rows == cols, 1.0, 0.0).astype(F32)

    def shifted(i, j):
        both = kept(pattern, tiles[i], tiles[j]) & (i < order) & (j < order)
        tile = raw[pl.ds(i * TILE, TILE), pl.ds(j * TILE, TILE)].astype(F32)
        tile = jnp.where(both, tile, 0.0)
        if i == j:
            tile = tile - jnp.where(i < order, potential, 0.0) * eye
        return tile

    largest = jnp.zeros((), F32)
    for i in range(MAXT):
        total = jnp.zeros((TILE, TILE), F32)
        for j in range(MAXT):
            copy(i, j).wait()
            tile = shifted(i, j)
            total = total + tile * tile
        largest = jnp.maximum(largest, jnp.max(jnp.sum(total, axis=1)))
    root = jnp.sqrt(jnp.full((8, TILE), largest + 1e-06, F32))
    inverse = 1.0 / (jnp.abs(potential) + 2.0 * root)
    inverse = inverse[0:1, :]
    for i in range(MAXT):
        for j in range(MAXT):
            x[pl.ds(i * TILE, TILE), pl.ds(j * TILE, TILE)] = (shifted(i, j) * inverse).astype(BF16)

    band = 256
    brow = lax.broadcasted_iota(jnp.int32, (band, N), 0)
    bcol = lax.broadcasted_iota(jnp.int32, (band, N), 1)

    def one(k, _):
        def square(b, _):
            here = pl.ds(pl.multiple_of(b * band, band), band)
            q = jnp.dot(x[here, :], x[...], preferred_element_type=F32)
            diag = jnp.where(brow + b * band == bcol, 1.5, 0.0)
            f[here, :] = (diag - 0.5 * q).astype(BF16)
            return 0

        def apply(b, _):
            here = pl.ds(pl.multiple_of(b * band, band), band)
            y = jnp.dot(x[here, :], f[...], preferred_element_type=F32)
            raw[here, :] = y.astype(BF16)
            return 0

        lax.fori_loop(0, N // band, square, 0)
        lax.fori_loop(0, N // band, apply, 0)
        x[...] = raw[...]
        return 0

    lax.fori_loop(0, 2, one, 0)
    head = pl.ds(0, TILE)
    prow = lax.broadcasted_iota(jnp.int32, (N, TILE), 0)
    pcol = lax.broadcasted_iota(jnp.int32, (N, TILE), 1)
    q = jnp.dot(x[...], x[:, head], preferred_element_type=F32)
    f[:, head] = (jnp.where(prow == pcol, 1.5, 0.0) - 0.5 * q).astype(BF16)
    y = jnp.dot(x[...], f[:, head], preferred_element_type=F32)
    dens = jnp.where(prow == pcol, 0.5, 0.0) - 0.5 * y
    for i in range(MAXT):
        d[:, pl.ds(i * TILE, TILE)] = dens[i * TILE : (i + 1) * TILE, :].T
    offset = pl.multiple_of(s % (TILE // CW) * CW, CW)
    groups[...] = jnp.zeros_like(groups)
    for i in range(MAXT):
        piece = d[pl.ds(offset, CW), pl.ds(i * TILE, TILE)].astype(BF16)
        panel[i] = piece

        @pl.when(i < order)
        def _():
            groups[tiles[i] // CT] = piece


def hp_kernel(ids, lists, orders, pattern, gathered, panels, hp, pt, strip):
    step = pl.program_id(0)

    @pl.when(step == 0)
    def _():
        pt[...] = jnp.zeros_like(pt)
        for k in range(ROWS):
            s = ids[1] * ROWS + k
            for i in range(MAXT):

                @pl.when(i < orders[s])
                def _():
                    where = pl.multiple_of(lists[s * MAXT + i] * TILE, TILE)
                    pt[pl.ds(k * CW, CW), pl.ds(where, TILE)] = panels[k, i]

    for c in range(COLS):
        for i in range(RT):
            for j in range(CT):
                b = c * CT + j
                live = kept(pattern, step * RT + i, b)

                @pl.when(live)
                def _():
                    strip[pl.ds(i * TILE, TILE), pl.ds(b * TILE, TILE)] = gathered[
                        c, pl.ds(i * TILE, TILE), pl.ds(j * TILE, TILE)
                    ]

                @pl.when(jnp.logical_not(live))
                def _():
                    strip[pl.ds(i * TILE, TILE), pl.ds(b * TILE, TILE)] = jnp.zeros(
                        (TILE, TILE), BF16
                    )

    hp[...] = lax.dot_general(
        strip[...], pt[...], (((1,), (1,)), ((), ())), preferred_element_type=F32
    ).astype(BF16)


def final_kernel(ids, present, arrived, hp, density, php, pt):
    def place(s, _):
        owner = s % ROWS * COLS + s // ROWS
        here = pl.ds(pl.multiple_of(s * CW, CW), CW)
        for a in range(RT):
            piece = arrived[owner, a // CT]
            live = present[s * RT + a] > 0
            pt[here, pl.ds(a * TILE, TILE)] = jnp.where(live, piece, jnp.zeros_like(piece))
        return 0

    lax.fori_loop(0, SUBS, place, 0)
    php[...] = lax.dot_general(
        pt[...], hp[...], (((0,), (0,)), ((), ())), preferred_element_type=F32
    )
    width = CT * TILE
    mine = pt[pl.ds(pl.multiple_of(ids[1] * width, width), width), :]
    density[...] = mine.T


def per_device(hamiltonian, pattern, tile_lists, orders, shift):
    row = lax.axis_index("row")
    col = lax.axis_index("col")
    ids = jnp.stack([row, col]).astype(jnp.int32)
    lists = tile_lists.reshape(-1)
    flat_pattern = pattern.reshape(-1)
    smem = pl.BlockSpec(memory_space=pltpu.SMEM)
    vmem = pl.BlockSpec(memory_space=pltpu.VMEM)
    gathered = lax.all_gather(hamiltonian, ("row", "col"), axis=0, tiled=False)
    panel, groups = pl.pallas_call(
        solve_kernel,
        out_shape=(
            jax.ShapeDtypeStruct((MAXT, CW, TILE), BF16),
            jax.ShapeDtypeStruct((NB // CT, CW, TILE), BF16),
        ),
        in_specs=[smem] * 5 + [pl.BlockSpec(memory_space=pl.ANY)],
        out_specs=(vmem, vmem),
        scratch_shapes=[
            pltpu.VMEM((N, N), BF16),
            pltpu.VMEM((N, N), BF16),
            pltpu.VMEM((N, N), BF16),
            pltpu.VMEM((TILE, N), F32),
            pltpu.SemaphoreType.DMA((MAXT, MAXT)),
        ],
        name="solve",
    )(ids, lists, orders, flat_pattern, shift, gathered)
    outgoing = jnp.broadcast_to(
        groups.reshape(ROWS, 1, CT, CW, TILE), (ROWS, COLS, CT, CW, TILE)
    ).reshape(SUBS, CT, CW, TILE)
    arrived = lax.all_to_all(outgoing, ("row", "col"), 0, 0, tiled=True)
    panels = lax.all_gather(panel, "row", axis=0, tiled=False)
    hp = pl.pallas_call(
        hp_kernel,
        out_shape=jax.ShapeDtypeStruct((NB * TILE, CT * TILE), BF16),
        grid_spec=pltpu.PrefetchScalarGridSpec(
            num_scalar_prefetch=4,
            grid=(ROWS,),
            in_specs=[
                pl.BlockSpec((COLS, RT * TILE, CT * TILE), lambda r, *_: (r, 0, 0)),
                pl.BlockSpec((ROWS, MAXT, CW, TILE), lambda r, *_: (0, 0, 0, 0)),
            ],
            out_specs=pl.BlockSpec((RT * TILE, CT * TILE), lambda r, *_: (r, 0)),
            scratch_shapes=[
                pltpu.VMEM((CT * TILE, NB * TILE), BF16),
                pltpu.VMEM((RT * TILE, NB * TILE), BF16),
            ],
        ),
        name="hp",
    )(ids, lists, orders, flat_pattern, gathered, panels)
    own = row * RT + jnp.arange(RT, dtype=jnp.int32)
    live = jnp.arange(MAXT, dtype=jnp.int32)[None, :] < orders[:, None]
    present = jnp.any((tile_lists[:, None, :] == own[None, :, None]) & live[:, None, :], axis=2)
    density, php = pl.pallas_call(
        final_kernel,
        out_shape=(
            jax.ShapeDtypeStruct((RT * TILE, CT * TILE), BF16),
            jax.ShapeDtypeStruct((RT * TILE, CT * TILE), F32),
        ),
        in_specs=[smem, smem, vmem, vmem],
        out_specs=(vmem, vmem),
        scratch_shapes=[pltpu.VMEM((NB * TILE, RT * TILE), BF16)],
        name="final",
    )(ids, present.astype(jnp.int32).reshape(-1), arrived, hp)
    return density, php


def solution(mesh):
    return jax.shard_map(
        per_device,
        mesh=mesh,
        in_specs=(P("row", "col"), P(), P(), P(), P()),
        out_specs=(P("row", "col"), P("row", "col")),
        check_vma=False,
    )
```

```python
import jax
import jax.numpy as jnp
from jax import lax
from jax.experimental import pallas as pl
from jax.experimental.pallas import tpu as pltpu
from jax.sharding import PartitionSpec as P

TILE = 128
MAXT = 8
NB = 32
ROWS = 8
COLS = 16
SUBS = 128
CW = 32
N = MAXT * TILE
RT = NB // ROWS
CT = NB // COLS
WIDTH = CT * TILE
F32 = jnp.float32
BF16 = jnp.bfloat16


def kept(pattern, a, b):
    return (pattern[a * NB + b] > 0) | (a == b)


def sent_to_all(x, axis, size):
    return lax.all_to_all(jnp.broadcast_to(x[None], (size, *x.shape)), axis, 0, 0, tiled=True)


def pack_kernel(ids, lists, orders, strip, out):
    def one(k, _):
        s = k * ROWS + ids[0]
        half = jnp.int32(-1)
        for j in range(MAXT):
            b = lists[s * MAXT + j]
            half = jnp.where((b // CT == ids[1]) & (j < orders[s]), b % CT, half)

        @pl.when(half >= 0)
        def _():
            lanes = pl.ds(pl.multiple_of(half * TILE, TILE), TILE)
            for i in range(MAXT):
                start = pl.multiple_of(lists[s * MAXT + i] * TILE, TILE)
                out[k, i] = strip[pl.ds(start, TILE), lanes]

        return 0

    lax.fori_loop(0, COLS, one, 0)


def solve_kernel(ids, lists, orders, pattern, shift, tiles, panel, x, f, y, d):
    s = ids[1] * ROWS + ids[0]
    order = orders[s]
    potential = shift[0]
    names = [lists[s * MAXT + j] for j in range(MAXT)]
    rows = lax.broadcasted_iota(jnp.int32, (TILE, TILE), 0)
    cols = lax.broadcasted_iota(jnp.int32, (TILE, TILE), 1)
    eye = jnp.where(rows == cols, 1.0, 0.0).astype(F32)

    def shifted(i, j):
        both = kept(pattern, names[i], names[j]) & (i < order) & (j < order)
        tile = jnp.where(both, tiles[names[j] // CT, i].astype(F32), 0.0)
        if i == j:
            tile = tile - jnp.where(i < order, potential, 0.0) * eye
        return tile

    largest = jnp.zeros((), F32)
    for i in range(MAXT):
        total = jnp.zeros((TILE, TILE), F32)
        for j in range(MAXT):
            tile = shifted(i, j)
            total = total + tile * tile
        largest = jnp.maximum(largest, jnp.max(jnp.sum(total, axis=1)))
    root = jnp.sqrt(jnp.full((8, TILE), largest + 1e-06, F32))
    inverse = (1.0 / (jnp.abs(potential) + 2.0 * root))[0:1, :]
    for i in range(MAXT):
        for j in range(MAXT):
            x[pl.ds(i * TILE, TILE), pl.ds(j * TILE, TILE)] = (shifted(i, j) * inverse).astype(BF16)

    band = 256
    brow = lax.broadcasted_iota(jnp.int32, (band, N), 0)
    bcol = lax.broadcasted_iota(jnp.int32, (band, N), 1)

    def step(source, target):
        def square(b, _):
            here = pl.ds(pl.multiple_of(b * band, band), band)
            q = jnp.dot(source[here, :], source[...], preferred_element_type=F32)
            diag = jnp.where(brow + b * band == bcol, 1.5, 0.0)
            f[here, :] = (diag - 0.5 * q).astype(BF16)
            return 0

        def apply(b, _):
            here = pl.ds(pl.multiple_of(b * band, band), band)
            target[here, :] = jnp.dot(
                source[here, :], f[...], preferred_element_type=F32
            ).astype(BF16)
            return 0

        lax.fori_loop(0, N // band, square, 0)
        lax.fori_loop(0, N // band, apply, 0)

    step(x, y)
    step(y, x)
    head = pl.ds(0, TILE)
    prow = lax.broadcasted_iota(jnp.int32, (N, TILE), 0)
    pcol = lax.broadcasted_iota(jnp.int32, (N, TILE), 1)
    q = jnp.dot(x[...], x[:, head], preferred_element_type=F32)
    f[:, head] = (jnp.where(prow == pcol, 1.5, 0.0) - 0.5 * q).astype(BF16)
    z = jnp.dot(x[...], f[:, head], preferred_element_type=F32)
    dens = jnp.where(prow == pcol, 0.5, 0.0) - 0.5 * z
    for i in range(MAXT):
        d[:, pl.ds(i * TILE, TILE)] = dens[i * TILE : (i + 1) * TILE, :].T
    offset = pl.multiple_of(s % (TILE // CW) * CW, CW)
    for i in range(MAXT):
        panel[i] = d[pl.ds(offset, CW), pl.ds(i * TILE, TILE)].astype(BF16)


def spread_kernel(ids, lists, orders, panels, out):
    out[...] = jnp.zeros_like(out)
    for k in range(ROWS):
        s = ids[1] * ROWS + k
        for i in range(MAXT):
            group = lists[s * MAXT + i] // CT

            @pl.when((i < orders[s]) & (group // (RT // CT) == ids[0]))
            def _():
                for c in range(COLS):
                    out[c, k, group % (RT // CT)] = panels[k, i]


def hp_kernel(ids, lists, orders, pattern, strip, panels, hp, pt, wide, sems):
    copies = [
        pltpu.make_async_copy(strip.at[c], wide.at[:, pl.ds(c * WIDTH, WIDTH)], sems.at[c])
        for c in range(COLS)
    ]
    for copy in copies:
        copy.start()
    pt[...] = jnp.zeros_like(pt)
    for k in range(ROWS):
        s = ids[1] * ROWS + k
        for i in range(MAXT):

            @pl.when(i < orders[s])
            def _():
                where = pl.multiple_of(lists[s * MAXT + i] * TILE, TILE)
                pt[pl.ds(k * CW, CW), pl.ds(where, TILE)] = panels[k, i]

    for copy in copies:
        copy.wait()

    def clear(b, _):
        lanes = pl.ds(pl.multiple_of(b * TILE, TILE), TILE)
        for a in range(RT):

            @pl.when(jnp.logical_not(kept(pattern, ids[0] * RT + a, b)))
            def _():
                wide[pl.ds(a * TILE, TILE), lanes] = jnp.zeros((TILE, TILE), BF16)

        return 0

    lax.fori_loop(0, NB, clear, 0)
    hp[...] = lax.dot_general(
        wide[...], pt[...], (((1,), (1,)), ((), ())), preferred_element_type=F32
    ).astype(BF16)


def final_kernel(ids, present, arrived, hp, density, php, pt):
    def place(s, _):
        here = pl.ds(pl.multiple_of(s * CW, CW), CW)
        for a in range(RT):
            piece = arrived[s, a // CT]
            live = present[s * RT + a] > 0
            pt[here, pl.ds(a * TILE, TILE)] = jnp.where(live, piece, jnp.zeros_like(piece))
        return 0

    lax.fori_loop(0, SUBS, place, 0)
    php[...] = lax.dot_general(
        pt[...], hp[...], (((0,), (0,)), ((), ())), preferred_element_type=F32
    )
    mine = pt[pl.ds(pl.multiple_of(ids[1] * WIDTH, WIDTH), WIDTH), :]
    density[...] = mine.T


def per_device(hamiltonian, pattern, tile_lists, orders, shift):
    row = lax.axis_index("row")
    col = lax.axis_index("col")
    ids = jnp.stack([row, col]).astype(jnp.int32)
    lists = tile_lists.reshape(-1)
    smem = pl.BlockSpec(memory_space=pltpu.SMEM)
    vmem = pl.BlockSpec(memory_space=pltpu.VMEM)
    hbm = pl.BlockSpec(memory_space=pl.ANY)
    flat_pattern = pattern.reshape(-1)
    row_strip = lax.all_gather(hamiltonian, "col", axis=0, tiled=False)
    col_strip = sent_to_all(hamiltonian, "row", ROWS).reshape(NB * TILE, WIDTH)
    packed = pl.pallas_call(
        pack_kernel,
        out_shape=jax.ShapeDtypeStruct((COLS, MAXT, TILE, TILE), BF16),
        in_specs=[smem, smem, smem, vmem],
        out_specs=vmem,
        name="pack",
    )(ids, lists, orders, col_strip)
    tiles = lax.all_to_all(packed, "col", 0, 0, tiled=True)
    panel = pl.pallas_call(
        solve_kernel,
        out_shape=jax.ShapeDtypeStruct((MAXT, CW, TILE), BF16),
        in_specs=[smem] * 5 + [vmem],
        out_specs=vmem,
        scratch_shapes=[
            pltpu.VMEM((N, N), BF16),
            pltpu.VMEM((N, N), BF16),
            pltpu.VMEM((N, N), BF16),
            pltpu.VMEM((TILE, N), F32),
        ],
        name="solve",
    )(ids, lists, orders, flat_pattern, shift, tiles)
    panels = lax.all_gather(panel, "row", axis=0, tiled=False)
    spread = pl.pallas_call(
        spread_kernel,
        out_shape=jax.ShapeDtypeStruct((COLS, ROWS, RT // CT, CW, TILE), BF16),
        in_specs=[smem] * 3 + [vmem],
        out_specs=vmem,
        name="spread",
    )(ids, lists, orders, panels)
    arrived = lax.all_to_all(spread, "col", 0, 0, tiled=True)
    hp = pl.pallas_call(
        hp_kernel,
        out_shape=jax.ShapeDtypeStruct((RT * TILE, WIDTH), BF16),
        in_specs=[smem] * 4 + [hbm, vmem],
        out_specs=vmem,
        scratch_shapes=[
            pltpu.VMEM((WIDTH, NB * TILE), BF16),
            pltpu.VMEM((RT * TILE, NB * TILE), BF16),
            pltpu.SemaphoreType.DMA((COLS,)),
        ],
        name="hp",
    )(ids, lists, orders, flat_pattern, row_strip, panels)
    hp_strip = sent_to_all(hp, "row", ROWS).reshape(NB * TILE, WIDTH)
    own = row * RT + jnp.arange(RT, dtype=jnp.int32)
    live = jnp.arange(MAXT, dtype=jnp.int32)[None, :] < orders[:, None]
    present = jnp.any((tile_lists[:, None, :] == own[None, :, None]) & live[:, None, :], axis=2)
    density, php = pl.pallas_call(
        final_kernel,
        out_shape=(
            jax.ShapeDtypeStruct((RT * TILE, WIDTH), BF16),
            jax.ShapeDtypeStruct((RT * TILE, WIDTH), F32),
        ),
        in_specs=[smem, smem, vmem, vmem],
        out_specs=(vmem, vmem),
        scratch_shapes=[pltpu.VMEM((NB * TILE, RT * TILE), BF16)],
        name="final",
    )(ids, present.astype(jnp.int32).reshape(-1), arrived.reshape(SUBS, RT // CT, CW, TILE), hp_strip)
    return density, php


def solution(mesh):
    return jax.shard_map(
        per_device,
        mesh=mesh,
        in_specs=(P("row", "col"), P(), P(), P(), P()),
        out_specs=(P("row", "col"), P("row", "col")),
        check_vma=False,
    )
```

```python
import jax
import jax.numpy as jnp
from jax import lax
from jax.experimental import pallas as pl
from jax.experimental.pallas import tpu as pltpu
from jax.sharding import Mesh
from jax.sharding import PartitionSpec as P

TILE = 128
MAXT = 8
NB = 32
ROWS = 8
COLS = 16
SUBS = 128
CW = 32
N = MAXT * TILE
RT = NB // ROWS
CT = NB // COLS
WIDTH = CT * TILE
ROW = ("z", "core")
COL = ("c0", "c1")
F32 = jnp.float32
BF16 = jnp.bfloat16


def kept(pattern, a, b):
    return (pattern[a * NB + b] > 0) | (a == b)


def sent_to_all(x, axis, size):
    return lax.all_to_all(jnp.broadcast_to(x[None], (size, *x.shape)), axis, 0, 0, tiled=True)


def pack_kernel(ids, lists, orders, strip, out):
    def one(k, _):
        s = k * ROWS + ids[0]
        half = jnp.int32(-1)
        for j in range(MAXT):
            b = lists[s * MAXT + j]
            half = jnp.where((b // CT == ids[1]) & (j < orders[s]), b % CT, half)

        @pl.when(half >= 0)
        def _():
            lanes = pl.ds(pl.multiple_of(half * TILE, TILE), TILE)
            for i in range(MAXT):
                start = pl.multiple_of(lists[s * MAXT + i] * TILE, TILE)
                out[k, i] = strip[pl.ds(start, TILE), lanes]

        return 0

    lax.fori_loop(0, COLS, one, 0)


def solve_kernel(ids, lists, orders, pattern, shift, tiles, panel, x, f, y, d):
    s = ids[1] * ROWS + ids[0]
    order = orders[s]
    potential = shift[0]
    names = [lists[s * MAXT + j] for j in range(MAXT)]
    rows = lax.broadcasted_iota(jnp.int32, (TILE, TILE), 0)
    cols = lax.broadcasted_iota(jnp.int32, (TILE, TILE), 1)
    eye = jnp.where(rows == cols, 1.0, 0.0).astype(F32)

    def shifted(i, j):
        both = kept(pattern, names[i], names[j]) & (i < order) & (j < order)
        tile = jnp.where(both, tiles[names[j] // CT, i].astype(F32), 0.0)
        if i == j:
            tile = tile - jnp.where(i < order, potential, 0.0) * eye
        return tile

    largest = jnp.zeros((), F32)
    for i in range(MAXT):
        total = jnp.zeros((TILE, TILE), F32)
        for j in range(MAXT):
            tile = shifted(i, j)
            total = total + tile * tile
        largest = jnp.maximum(largest, jnp.max(jnp.sum(total, axis=1)))
    root = jnp.sqrt(jnp.full((8, TILE), largest + 1e-06, F32))
    inverse = (1.0 / (jnp.abs(potential) + 2.0 * root))[0:1, :]
    for i in range(MAXT):
        for j in range(MAXT):
            x[pl.ds(i * TILE, TILE), pl.ds(j * TILE, TILE)] = (shifted(i, j) * inverse).astype(BF16)

    band = 256
    brow = lax.broadcasted_iota(jnp.int32, (band, N), 0)
    bcol = lax.broadcasted_iota(jnp.int32, (band, N), 1)

    def step(source, target):
        def square(b, _):
            here = pl.ds(pl.multiple_of(b * band, band), band)
            q = jnp.dot(source[here, :], source[...], preferred_element_type=F32)
            diag = jnp.where(brow + b * band == bcol, 1.5, 0.0)
            f[here, :] = (diag - 0.5 * q).astype(BF16)
            return 0

        def apply(b, _):
            here = pl.ds(pl.multiple_of(b * band, band), band)
            target[here, :] = jnp.dot(
                source[here, :], f[...], preferred_element_type=F32
            ).astype(BF16)
            return 0

        lax.fori_loop(0, N // band, square, 0)
        lax.fori_loop(0, N // band, apply, 0)

    step(x, y)
    step(y, x)
    head = pl.ds(0, TILE)
    prow = lax.broadcasted_iota(jnp.int32, (N, TILE), 0)
    pcol = lax.broadcasted_iota(jnp.int32, (N, TILE), 1)
    q = jnp.dot(x[...], x[:, head], preferred_element_type=F32)
    f[:, head] = (jnp.where(prow == pcol, 1.5, 0.0) - 0.5 * q).astype(BF16)
    z = jnp.dot(x[...], f[:, head], preferred_element_type=F32)
    dens = jnp.where(prow == pcol, 0.5, 0.0) - 0.5 * z
    for i in range(MAXT):
        d[:, pl.ds(i * TILE, TILE)] = dens[i * TILE : (i + 1) * TILE, :].T
    offset = pl.multiple_of(s % (TILE // CW) * CW, CW)
    for i in range(MAXT):
        panel[i] = d[pl.ds(offset, CW), pl.ds(i * TILE, TILE)].astype(BF16)


def spread_kernel(ids, lists, orders, panels, out):
    out[...] = jnp.zeros_like(out)
    for k in range(ROWS):
        s = ids[1] * ROWS + k
        for i in range(MAXT):
            group = lists[s * MAXT + i] // CT

            @pl.when((i < orders[s]) & (group // (RT // CT) == ids[0]))
            def _():
                for c in range(COLS):
                    out[c, k, group % (RT // CT)] = panels[k, i]


def hp_kernel(ids, lists, orders, pattern, a0, a1, a2, a3, b0, b1, b2, b3, panels, hp, pt, wide, sems):
    half = RT * TILE // 2
    c0 = ids[1] // 4
    c1 = ids[1] % 4
    copies = []
    for k in range(4):
        for m in range(4):
            first = (c0 + k) % 4 * 4 + (c1 + m) % 4
            second = (c0 + m) % 4 * 4 + (c1 + k) % 4
            for part, ref, col in ((0, (a0, a1, a2, a3)[k], first), (1, (b0, b1, b2, b3)[k], second)):
                lanes = pl.ds(pl.multiple_of(col * WIDTH, WIDTH), WIDTH)
                copies.append(
                    pltpu.make_async_copy(
                        ref.at[m], wide.at[pl.ds(part * half, half), lanes], sems.at[part, k, m]
                    )
                )
    for copy in copies:
        copy.start()
    pt[...] = jnp.zeros_like(pt)
    for k in range(ROWS):
        s = ids[1] * ROWS + k
        for i in range(MAXT):

            @pl.when(i < orders[s])
            def _():
                where = pl.multiple_of(lists[s * MAXT + i] * TILE, TILE)
                pt[pl.ds(k * CW, CW), pl.ds(where, TILE)] = panels[k, i]

    for copy in copies:
        copy.wait()

    def clear(b, _):
        lanes = pl.ds(pl.multiple_of(b * TILE, TILE), TILE)
        for a in range(RT):

            @pl.when(jnp.logical_not(kept(pattern, ids[0] * RT + a, b)))
            def _():
                wide[pl.ds(a * TILE, TILE), lanes] = jnp.zeros((TILE, TILE), BF16)

        return 0

    lax.fori_loop(0, NB, clear, 0)
    hp[...] = lax.dot_general(
        wide[...], pt[...], (((1,), (1,)), ((), ())), preferred_element_type=F32
    ).astype(BF16)


def place_kernel(ids, present, arrived, density, pt):
    def place(s, _):
        here = pl.ds(pl.multiple_of(s * CW, CW), CW)
        for a in range(RT):
            piece = arrived[s, a // CT]
            live = present[s * RT + a] > 0
            pt[here, pl.ds(a * TILE, TILE)] = jnp.where(live, piece, jnp.zeros_like(piece))
        return 0

    lax.fori_loop(0, SUBS, place, 0)
    mine = pt[pl.ds(pl.multiple_of(ids[1] * WIDTH, WIDTH), WIDTH), :]
    density[...] = mine.T


def php_kernel(ids, pt, m0, m1, m2, m3, o0, o1, o2, o3, php, hp, sems):
    z = ids[0] // 2
    core = ids[0] % 2
    copies = []
    for k in range(4):
        for part, ref in ((0, (m0, m1, m2, m3)[k]), (1, (o0, o1, o2, o3)[k])):
            owner = (z + k) % 4 * 2 + (core + part) % 2
            rows = pl.ds(pl.multiple_of(owner * RT * TILE, RT * TILE), RT * TILE)
            copies.append(pltpu.make_async_copy(ref, hp.at[rows, :], sems.at[part, k]))
    for copy in copies:
        copy.start()
    for copy in copies:
        copy.wait()
    php[...] = lax.dot_general(
        pt[...], hp[...], (((0,), (0,)), ((), ())), preferred_element_type=F32
    )


def from_ring(x, axis):
    return [x] + [lax.ppermute(x, axis, [((i + k) % 4, i) for i in range(4)]) for k in range(1, 4)]


def per_device(hamiltonian, pattern, tile_lists, orders, shift):
    row = lax.axis_index(ROW)
    col = lax.axis_index(COL)
    ids = jnp.stack([row, col]).astype(jnp.int32)
    lists = tile_lists.reshape(-1)
    smem = pl.BlockSpec(memory_space=pltpu.SMEM)
    vmem = pl.BlockSpec(memory_space=pltpu.VMEM)
    hbm = pl.BlockSpec(memory_space=pl.ANY)
    flat_pattern = pattern.reshape(-1)
    half = RT * TILE // 2
    ahead = from_ring(hamiltonian[:half], "c1")
    across = from_ring(hamiltonian[half:], "c0")
    col_strip = sent_to_all(hamiltonian, ROW, ROWS).reshape(NB * TILE, WIDTH)
    ahead = from_ring(jnp.stack(ahead), "c0")
    across = from_ring(jnp.stack(across), "c1")
    packed = pl.pallas_call(
        pack_kernel,
        out_shape=jax.ShapeDtypeStruct((COLS, MAXT, TILE, TILE), BF16),
        in_specs=[smem, smem, smem, vmem],
        out_specs=vmem,
        name="pack",
    )(ids, lists, orders, col_strip)
    packed, ahead, across = lax.optimization_barrier((packed, ahead, across))
    tiles = lax.all_to_all(packed, COL, 0, 0, tiled=True)
    panel = pl.pallas_call(
        solve_kernel,
        out_shape=jax.ShapeDtypeStruct((MAXT, CW, TILE), BF16),
        in_specs=[smem] * 5 + [vmem],
        out_specs=vmem,
        scratch_shapes=[
            pltpu.VMEM((N, N), BF16),
            pltpu.VMEM((N, N), BF16),
            pltpu.VMEM((N, N), BF16),
            pltpu.VMEM((TILE, N), F32),
        ],
        name="solve",
    )(ids, lists, orders, flat_pattern, shift, tiles)
    panels = lax.all_gather(panel, ROW, axis=0, tiled=False)
    spread = pl.pallas_call(
        spread_kernel,
        out_shape=jax.ShapeDtypeStruct((COLS, ROWS, RT // CT, CW, TILE), BF16),
        in_specs=[smem] * 3 + [vmem],
        out_specs=vmem,
        name="spread",
    )(ids, lists, orders, panels)
    arrived = lax.all_to_all(spread, COL, 0, 0, tiled=True)
    hp = pl.pallas_call(
        hp_kernel,
        out_shape=jax.ShapeDtypeStruct((RT * TILE, WIDTH), BF16),
        in_specs=[smem] * 4 + [hbm] * 8 + [vmem],
        out_specs=vmem,
        scratch_shapes=[
            pltpu.VMEM((WIDTH, NB * TILE), BF16),
            pltpu.VMEM((RT * TILE, NB * TILE), BF16),
            pltpu.SemaphoreType.DMA((2, 4, 4)),
        ],
        name="hp",
    )(ids, lists, orders, flat_pattern, *ahead, *across, panels)
    ours = from_ring(hp, "z")
    theirs = [lax.ppermute(x, "core", [(0, 1), (1, 0)]) for x in ours]
    own = row * RT + jnp.arange(RT, dtype=jnp.int32)
    live = jnp.arange(MAXT, dtype=jnp.int32)[None, :] < orders[:, None]
    present = jnp.any((tile_lists[:, None, :] == own[None, :, None]) & live[:, None, :], axis=2)
    density, pt = pl.pallas_call(
        place_kernel,
        out_shape=(
            jax.ShapeDtypeStruct((RT * TILE, WIDTH), BF16),
            jax.ShapeDtypeStruct((NB * TILE, RT * TILE), BF16),
        ),
        in_specs=[smem, smem, vmem],
        out_specs=(vmem, vmem),
        name="place",
    )(ids, present.astype(jnp.int32).reshape(-1), arrived.reshape(SUBS, RT // CT, CW, TILE))
    php = pl.pallas_call(
        php_kernel,
        out_shape=jax.ShapeDtypeStruct((RT * TILE, WIDTH), F32),
        in_specs=[smem, vmem] + [hbm] * 8,
        out_specs=vmem,
        scratch_shapes=[pltpu.VMEM((NB * TILE, WIDTH), BF16), pltpu.SemaphoreType.DMA((2, 4))],
        name="php",
    )(ids, pt, *ours, *theirs)
    return density, php


def solution(mesh):
    fine = Mesh(mesh.devices.reshape(4, 2, 4, 4), ("z", "core", "c0", "c1"))
    split = P(ROW, COL)
    return jax.shard_map(
        per_device,
        mesh=fine,
        in_specs=(split, P(), P(), P(), P()),
        out_specs=(split, split),
        check_vma=False,
    )
```

```python
import jax
import jax.numpy as jnp
from jax import lax
from jax.experimental import pallas as pl
from jax.experimental.pallas import tpu as pltpu
from jax.sharding import Mesh
from jax.sharding import PartitionSpec as P

TILE = 128
MAXT = 8
NB = 32
ROWS = 8
COLS = 16
SUBS = 128
CW = 32
N = MAXT * TILE
RT = NB // ROWS
CT = NB // COLS
WIDTH = CT * TILE
ROW = ("z", "core")
COL = ("c0", "c1")
F32 = jnp.float32
BF16 = jnp.bfloat16


def kept(pattern, a, b):
    return (pattern[a * NB + b] > 0) | (a == b)


def ring_owner(ids, k, part):
    return (ids[0] // 2 + k) % 4 * 2 + (ids[0] + part) % 2


def row_copies(ids, blocks, whole, sems):
    copies = []
    for part in range(2):
        for k in range(4):
            rows = pl.ds(pl.multiple_of(ring_owner(ids, k, part) * RT * TILE, RT * TILE), RT * TILE)
            copies.append(
                pltpu.make_async_copy(blocks[part * 4 + k], whole.at[rows, :], sems.at[part, k])
            )
    return copies


def pack_kernel(ids, lists, orders, *refs):
    blocks, (out, strip, sems) = refs[:8], refs[8:]
    copies = row_copies(ids, blocks, strip, sems)
    for copy in copies:
        copy.start()
    for copy in copies:
        copy.wait()

    def one(k, _):
        s = k * ROWS + ids[0]
        half = jnp.int32(-1)
        for j in range(MAXT):
            b = lists[s * MAXT + j]
            half = jnp.where((b // CT == ids[1]) & (j < orders[s]), b % CT, half)

        @pl.when(half >= 0)
        def _():
            lanes = pl.ds(pl.multiple_of(half * TILE, TILE), TILE)
            for i in range(MAXT):
                start = pl.multiple_of(lists[s * MAXT + i] * TILE, TILE)
                out[k, i] = strip[pl.ds(start, TILE), lanes]

        return 0

    lax.fori_loop(0, COLS, one, 0)


def solve_kernel(ids, lists, orders, pattern, shift, tiles, panel, x, f, y, d):
    s = ids[1] * ROWS + ids[0]
    order = orders[s]
    potential = shift[0]
    names = [lists[s * MAXT + j] for j in range(MAXT)]
    rows = lax.broadcasted_iota(jnp.int32, (TILE, TILE), 0)
    cols = lax.broadcasted_iota(jnp.int32, (TILE, TILE), 1)
    eye = jnp.where(rows == cols, 1.0, 0.0).astype(F32)

    def shifted(i, j):
        both = kept(pattern, names[i], names[j]) & (i < order) & (j < order)
        tile = jnp.where(both, tiles[names[j] // CT, i].astype(F32), 0.0)
        if i == j:
            tile = tile - jnp.where(i < order, potential, 0.0) * eye
        return tile

    largest = jnp.zeros((), F32)
    for i in range(MAXT):
        total = jnp.zeros((TILE, TILE), F32)
        for j in range(MAXT):
            tile = shifted(i, j)
            total = total + tile * tile
        largest = jnp.maximum(largest, jnp.max(jnp.sum(total, axis=1)))
    root = jnp.sqrt(jnp.full((8, TILE), largest + 1e-06, F32))
    inverse = (1.0 / (jnp.abs(potential) + 2.0 * root))[0:1, :]
    for i in range(MAXT):
        for j in range(MAXT):
            x[pl.ds(i * TILE, TILE), pl.ds(j * TILE, TILE)] = (shifted(i, j) * inverse).astype(BF16)

    band = 512
    brow = lax.broadcasted_iota(jnp.int32, (band, N), 0)
    bcol = lax.broadcasted_iota(jnp.int32, (band, N), 1)

    def step(source, target):
        def square(b, _):
            here = pl.ds(pl.multiple_of(b * band, band), band)
            q = jnp.dot(source[here, :], source[...], preferred_element_type=F32)
            diag = jnp.where(brow + b * band == bcol, 1.5, 0.0)
            f[here, :] = (diag - 0.5 * q).astype(BF16)
            return 0

        def apply(b, _):
            here = pl.ds(pl.multiple_of(b * band, band), band)
            target[here, :] = jnp.dot(
                source[here, :], f[...], preferred_element_type=F32
            ).astype(BF16)
            return 0

        lax.fori_loop(0, N // band, square, 0)
        lax.fori_loop(0, N // band, apply, 0)

    step(x, y)
    step(y, x)
    head = pl.ds(0, TILE)
    prow = lax.broadcasted_iota(jnp.int32, (N, TILE), 0)
    pcol = lax.broadcasted_iota(jnp.int32, (N, TILE), 1)
    q = jnp.dot(x[...], x[:, head], preferred_element_type=F32)
    f[:, head] = (jnp.where(prow == pcol, 1.5, 0.0) - 0.5 * q).astype(BF16)
    z = jnp.dot(x[...], f[:, head], preferred_element_type=F32)
    dens = jnp.where(prow == pcol, 0.5, 0.0) - 0.5 * z
    for i in range(MAXT):
        d[:, pl.ds(i * TILE, TILE)] = dens[i * TILE : (i + 1) * TILE, :].T
    offset = pl.multiple_of(s % (TILE // CW) * CW, CW)
    for i in range(MAXT):
        panel[i] = d[pl.ds(offset, CW), pl.ds(i * TILE, TILE)].astype(BF16)


def spread_kernel(ids, lists, orders, p0, p1, p2, p3, even, odd):
    even[...] = jnp.zeros_like(even)
    odd[...] = jnp.zeros_like(odd)
    for z in range(4):
        for part in range(2):
            k = ring_owner(ids, z, part)
            s = ids[1] * ROWS + k
            for i in range(MAXT):
                group = lists[s * MAXT + i] // CT
                live = i < orders[s]

                @pl.when(live & (group == 2 * ids[0]))
                def _():
                    even[k] = (p0, p1, p2, p3)[z][part, i]

                @pl.when(live & (group == 2 * ids[0] + 1))
                def _():
                    odd[k] = (p0, p1, p2, p3)[z][part, i]


def hp_kernel(ids, lists, orders, pattern, a0, a1, a2, a3, b0, b1, b2, b3, p0, p1, p2, p3, hp, pt, wide, sems):
    half = RT * TILE // 2
    c0 = ids[1] // 4
    c1 = ids[1] % 4
    copies = []
    for k in range(4):
        for m in range(4):
            first = (c0 + k) % 4 * 4 + (c1 + m) % 4
            second = (c0 + m) % 4 * 4 + (c1 + k) % 4
            for part, ref, col in ((0, (a0, a1, a2, a3)[k], first), (1, (b0, b1, b2, b3)[k], second)):
                lanes = pl.ds(pl.multiple_of(col * WIDTH, WIDTH), WIDTH)
                copies.append(
                    pltpu.make_async_copy(
                        ref.at[m], wide.at[pl.ds(part * half, half), lanes], sems.at[part, k, m]
                    )
                )
    for copy in copies:
        copy.start()
    pt[...] = jnp.zeros_like(pt)
    for z in range(4):
        for part in range(2):
            k = ring_owner(ids, z, part)
            s = ids[1] * ROWS + k
            here = pl.ds(pl.multiple_of(k * CW, CW), CW)
            for i in range(MAXT):

                @pl.when(i < orders[s])
                def _():
                    where = pl.multiple_of(lists[s * MAXT + i] * TILE, TILE)
                    pt[here, pl.ds(where, TILE)] = (p0, p1, p2, p3)[z][part, i]

    for copy in copies:
        copy.wait()

    def clear(b, _):
        lanes = pl.ds(pl.multiple_of(b * TILE, TILE), TILE)
        for a in range(RT):

            @pl.when(jnp.logical_not(kept(pattern, ids[0] * RT + a, b)))
            def _():
                wide[pl.ds(a * TILE, TILE), lanes] = jnp.zeros((TILE, TILE), BF16)

        return 0

    lax.fori_loop(0, NB, clear, 0)
    hp[...] = lax.dot_general(
        wide[...], pt[...], (((1,), (1,)), ((), ())), preferred_element_type=F32
    ).astype(BF16)


def final_kernel(ids, present, *refs):
    pieces, blocks = refs[:8], refs[8:16]
    density, php, pt, arrived, hp, sems = refs[16:]
    copies = row_copies(ids, blocks, hp, sems)
    panels = [
        pltpu.make_async_copy(pieces[g * 4 + k], arrived.at[g, k], sems.at[2 + g, k])
        for g in range(2)
        for k in range(4)
    ]
    for copy in panels + copies:
        copy.start()
    for copy in panels:
        copy.wait()
    c0 = ids[1] // 4
    c1 = ids[1] % 4
    for g in range(2):
        for k in range(4):

            def place(m, _):
                near, far = (c1 + m) % 4, (c0 + k) % 4
                if g == 1:
                    near, far = (c1 + k) % 4, (c0 + m) % 4
                s = (far * 4 + near) * ROWS
                for r in range(ROWS):
                    here = pl.ds(pl.multiple_of((s + r) * CW, CW), CW)
                    piece = arrived[g, k, m, r]
                    for a in range(CT):
                        live = present[(s + r) * RT + g * CT + a] > 0
                        lanes = pl.ds((g * CT + a) * TILE, TILE)
                        pt[here, lanes] = jnp.where(live, piece, jnp.zeros_like(piece))
                return 0

            lax.fori_loop(0, 4, place, 0)
    for copy in copies:
        copy.wait()
    php[...] = lax.dot_general(
        pt[...], hp[...], (((0,), (0,)), ((), ())), preferred_element_type=F32
    )
    mine = pt[pl.ds(pl.multiple_of(ids[1] * WIDTH, WIDTH), WIDTH), :]
    density[...] = mine.T


def from_ring(x, axis):
    return [x] + [lax.ppermute(x, axis, [((i + k) % 4, i) for i in range(4)]) for k in range(1, 4)]


def swapped(x):
    return lax.ppermute(x, "core", [(0, 1), (1, 0)])


def per_device(hamiltonian, pattern, tile_lists, orders, shift):
    row = lax.axis_index(ROW)
    col = lax.axis_index(COL)
    ids = jnp.stack([row, col]).astype(jnp.int32)
    lists = tile_lists.reshape(-1)
    smem = pl.BlockSpec(memory_space=pltpu.SMEM)
    vmem = pl.BlockSpec(memory_space=pltpu.VMEM)
    hbm = pl.BlockSpec(memory_space=pl.ANY)
    flat_pattern = pattern.reshape(-1)
    half = RT * TILE // 2
    ahead = from_ring(hamiltonian[:half], "c1")
    across = from_ring(hamiltonian[half:], "c0")
    strip = from_ring(hamiltonian, "z")
    strip = strip + [swapped(x) for x in strip]
    ahead = from_ring(jnp.stack(ahead), "c0")
    across = from_ring(jnp.stack(across), "c1")
    packed = pl.pallas_call(
        pack_kernel,
        out_shape=jax.ShapeDtypeStruct((COLS, MAXT, TILE, TILE), BF16),
        in_specs=[smem, smem, smem] + [hbm] * 8,
        out_specs=vmem,
        scratch_shapes=[pltpu.VMEM((NB * TILE, WIDTH), BF16), pltpu.SemaphoreType.DMA((2, 4))],
        name="pack",
    )(ids, lists, orders, *strip)
    packed, ahead, across = lax.optimization_barrier((packed, ahead, across))
    tiles = lax.all_to_all(packed, COL, 0, 0, tiled=True)
    panel = pl.pallas_call(
        solve_kernel,
        out_shape=jax.ShapeDtypeStruct((MAXT, CW, TILE), BF16),
        in_specs=[smem] * 5 + [vmem],
        out_specs=vmem,
        scratch_shapes=[
            pltpu.VMEM((N, N), BF16),
            pltpu.VMEM((N, N), BF16),
            pltpu.VMEM((N, N), BF16),
            pltpu.VMEM((TILE, N), F32),
        ],
        name="solve",
    )(ids, lists, orders, flat_pattern, shift, tiles)
    panels = from_ring(jnp.stack([panel, swapped(panel)]), "z")
    half_panels = jax.ShapeDtypeStruct((ROWS, CW, TILE), BF16)
    even, odd = pl.pallas_call(
        spread_kernel,
        out_shape=(half_panels, half_panels),
        in_specs=[smem] * 3 + [vmem] * 4,
        out_specs=(vmem, vmem),
        name="spread",
    )(ids, lists, orders, *panels)
    even = from_ring(jnp.stack(from_ring(even, "c1")), "c0")
    odd = from_ring(jnp.stack(from_ring(odd, "c0")), "c1")
    hp = pl.pallas_call(
        hp_kernel,
        out_shape=jax.ShapeDtypeStruct((RT * TILE, WIDTH), BF16),
        in_specs=[smem] * 4 + [hbm] * 8 + [vmem] * 4,
        out_specs=vmem,
        scratch_shapes=[
            pltpu.VMEM((WIDTH, NB * TILE), BF16),
            pltpu.VMEM((RT * TILE, NB * TILE), BF16),
            pltpu.SemaphoreType.DMA((2, 4, 4)),
        ],
        name="hp",
    )(ids, lists, orders, flat_pattern, *ahead, *across, *panels)
    ours = from_ring(hp, "z")
    theirs = [swapped(x) for x in ours]
    own = row * RT + jnp.arange(RT, dtype=jnp.int32)
    live = jnp.arange(MAXT, dtype=jnp.int32)[None, :] < orders[:, None]
    present = jnp.any((tile_lists[:, None, :] == own[None, :, None]) & live[:, None, :], axis=2)
    density, php = pl.pallas_call(
        final_kernel,
        out_shape=(
            jax.ShapeDtypeStruct((RT * TILE, WIDTH), BF16),
            jax.ShapeDtypeStruct((RT * TILE, WIDTH), F32),
        ),
        in_specs=[smem, smem] + [hbm] * 16,
        out_specs=(vmem, vmem),
        scratch_shapes=[
            pltpu.VMEM((NB * TILE, RT * TILE), BF16),
            pltpu.VMEM((2, 4, 4, ROWS, CW, TILE), BF16),
            pltpu.VMEM((NB * TILE, WIDTH), BF16),
            pltpu.SemaphoreType.DMA((4, 4)),
        ],
        name="final",
    )(ids, present.astype(jnp.int32).reshape(-1), *even, *odd, *ours, *theirs)
    return density, php


def solution(mesh):
    fine = Mesh(mesh.devices.reshape(4, 2, 4, 4), ("z", "core", "c0", "c1"))
    split = P(ROW, COL)
    return jax.shard_map(
        per_device,
        mesh=fine,
        in_specs=(split, P(), P(), P(), P()),
        out_specs=(split, split),
        check_vma=False,
    )
```

```python
import jax
import jax.numpy as jnp
from jax import lax
from jax.experimental import pallas as pl
from jax.experimental.pallas import tpu as pltpu
from jax.sharding import Mesh
from jax.sharding import PartitionSpec as P

TILE = 128
MAXT = 8
NB = 32
ROWS = 8
COLS = 16
SUBS = 128
CW = 32
N = MAXT * TILE
RT = NB // ROWS
CT = NB // COLS
WIDTH = CT * TILE
ROW = ("z", "core")
COL = ("c0", "c1")
F32 = jnp.float32
BF16 = jnp.bfloat16


def kept(pattern, a, b):
    return (pattern[a * NB + b] > 0) | (a == b)


def ring_owner(ids, k, part):
    return (ids[0] // 2 + k) % 4 * 2 + (ids[0] + part) % 2


def row_copies(ids, blocks, whole, sems):
    copies = []
    for part in range(2):
        for k in range(4):
            rows = pl.ds(pl.multiple_of(ring_owner(ids, k, part) * RT * TILE, RT * TILE), RT * TILE)
            copies.append(
                pltpu.make_async_copy(blocks[part * 4 + k], whole.at[rows, :], sems.at[part, k])
            )
    return copies


def cyclic(j, k):
    return 1 + (j - 1 + k) % (MAXT - 1)


def pack_kernel(ids, lists, orders, *refs):
    blocks, (out, first, strip, sems) = refs[:8], refs[8:]
    copies = row_copies(ids, blocks, strip, sems)
    for copy in copies:
        copy.start()
    for copy in copies:
        copy.wait()

    def tile(a, lanes):
        return strip[pl.ds(pl.multiple_of(a * TILE, TILE), TILE), lanes]

    own = (ids[1] * ROWS + ids[0]) * MAXT
    lanes = pl.ds(pl.multiple_of(lists[own] % CT * TILE, TILE), TILE)
    for i in range(MAXT):
        first[i] = tile(lists[own + i], lanes)

    def one(c, _):
        s = c * ROWS + ids[0]
        for j in range(1, MAXT):
            b = lists[s * MAXT + j]

            @pl.when((b // CT == ids[1]) & (j < orders[s]))
            def _():
                lanes = pl.ds(pl.multiple_of(b % CT * TILE, TILE), TILE)
                for k in range(4):
                    out[c, k] = tile(lists[s * MAXT + cyclic(j, k)], lanes)

        return 0

    lax.fori_loop(0, COLS, one, 0)


def solve_kernel(ids, lists, orders, pattern, shift, tiles, first, panel, x, f, y, d):
    s = ids[1] * ROWS + ids[0]
    order = orders[s]
    potential = shift[0]
    names = [lists[s * MAXT + j] for j in range(MAXT)]
    rows = lax.broadcasted_iota(jnp.int32, (TILE, TILE), 0)
    cols = lax.broadcasted_iota(jnp.int32, (TILE, TILE), 1)
    eye = jnp.where(rows == cols, 1.0, 0.0).astype(F32)

    def put(i, j, tile):
        y[pl.ds(i * TILE, TILE), pl.ds(j * TILE, TILE)] = tile

    for i in range(MAXT):
        put(i, 0, first[i])
        if i:
            put(0, i, first[i].T)
            for k in range(4):
                tile = tiles[names[i] // CT, k]
                put(cyclic(i, k), i, tile)
                if k:
                    put(i, cyclic(i, k), tile.T)

    def shifted(i, j):
        both = kept(pattern, names[i], names[j]) & (i < order) & (j < order)
        tile = y[pl.ds(i * TILE, TILE), pl.ds(j * TILE, TILE)].astype(F32)
        tile = jnp.where(both, tile, 0.0)
        if i == j:
            tile = tile - jnp.where(i < order, potential, 0.0) * eye
        return tile

    largest = jnp.zeros((), F32)
    for i in range(MAXT):
        total = jnp.zeros((TILE, TILE), F32)
        for j in range(MAXT):
            tile = shifted(i, j)
            total = total + tile * tile
        largest = jnp.maximum(largest, jnp.max(jnp.sum(total, axis=1)))
    root = jnp.sqrt(jnp.full((8, TILE), largest + 1e-06, F32))
    inverse = (1.0 / (jnp.abs(potential) + 2.0 * root))[0:1, :]
    for i in range(MAXT):
        for j in range(MAXT):
            x[pl.ds(i * TILE, TILE), pl.ds(j * TILE, TILE)] = (shifted(i, j) * inverse).astype(BF16)

    band = 512
    brow = lax.broadcasted_iota(jnp.int32, (band, N), 0)
    bcol = lax.broadcasted_iota(jnp.int32, (band, N), 1)

    def step(source, target):
        def square(b, _):
            here = pl.ds(pl.multiple_of(b * band, band), band)
            q = jnp.dot(source[here, :], source[...], preferred_element_type=F32)
            diag = jnp.where(brow + b * band == bcol, 1.5, 0.0)
            f[here, :] = (diag - 0.5 * q).astype(BF16)
            return 0

        def apply(b, _):
            here = pl.ds(pl.multiple_of(b * band, band), band)
            target[here, :] = jnp.dot(
                source[here, :], f[...], preferred_element_type=F32
            ).astype(BF16)
            return 0

        lax.fori_loop(0, N // band, square, 0)
        lax.fori_loop(0, N // band, apply, 0)

    step(x, y)
    step(y, x)
    head = pl.ds(0, TILE)
    prow = lax.broadcasted_iota(jnp.int32, (N, TILE), 0)
    pcol = lax.broadcasted_iota(jnp.int32, (N, TILE), 1)
    q = jnp.dot(x[...], x[:, head], preferred_element_type=F32)
    f[:, head] = (jnp.where(prow == pcol, 1.5, 0.0) - 0.5 * q).astype(BF16)
    z = jnp.dot(x[...], f[:, head], preferred_element_type=F32)
    dens = jnp.where(prow == pcol, 0.5, 0.0) - 0.5 * z
    for i in range(MAXT):
        d[:, pl.ds(i * TILE, TILE)] = dens[i * TILE : (i + 1) * TILE, :].T
    offset = pl.multiple_of(s % (TILE // CW) * CW, CW)
    for i in range(MAXT):
        panel[i] = d[pl.ds(offset, CW), pl.ds(i * TILE, TILE)].astype(BF16)


def spread_kernel(ids, lists, orders, panels, out, mine):
    mine[...] = jnp.zeros_like(mine)
    for k in range(ROWS):
        s = ids[1] * ROWS + k
        for i in range(MAXT):
            group = lists[s * MAXT + i] // CT

            @pl.when((i < orders[s]) & (group // (RT // CT) == ids[0]))
            def _():
                mine[k, group % (RT // CT)] = panels[k, i]

    def one(c, _):
        out[c] = mine[...]
        return 0

    lax.fori_loop(0, COLS, one, 0)


def hp_kernel(ids, lists, orders, pattern, a0, a1, a2, a3, b0, b1, b2, b3, panels, hp, pt, wide, sems):
    half = RT * TILE // 2
    c0 = ids[1] // 4
    c1 = ids[1] % 4
    copies = []
    for k in range(4):
        for m in range(4):
            first = (c0 + k) % 4 * 4 + (c1 + m) % 4
            second = (c0 + m) % 4 * 4 + (c1 + k) % 4
            for part, ref, col in ((0, (a0, a1, a2, a3)[k], first), (1, (b0, b1, b2, b3)[k], second)):
                lanes = pl.ds(pl.multiple_of(col * WIDTH, WIDTH), WIDTH)
                copies.append(
                    pltpu.make_async_copy(
                        ref.at[m], wide.at[pl.ds(part * half, half), lanes], sems.at[part, k, m]
                    )
                )
    for copy in copies:
        copy.start()
    pt[...] = jnp.zeros_like(pt)
    for k in range(ROWS):
        s = ids[1] * ROWS + k
        for i in range(MAXT):

            @pl.when(i < orders[s])
            def _():
                where = pl.multiple_of(lists[s * MAXT + i] * TILE, TILE)
                pt[pl.ds(k * CW, CW), pl.ds(where, TILE)] = panels[k, i]

    for copy in copies:
        copy.wait()

    def clear(b, _):
        lanes = pl.ds(pl.multiple_of(b * TILE, TILE), TILE)
        for a in range(RT):

            @pl.when(jnp.logical_not(kept(pattern, ids[0] * RT + a, b)))
            def _():
                wide[pl.ds(a * TILE, TILE), lanes] = jnp.zeros((TILE, TILE), BF16)

        return 0

    lax.fori_loop(0, NB, clear, 0)
    hp[...] = lax.dot_general(
        wide[...], pt[...], (((1,), (1,)), ((), ())), preferred_element_type=F32
    ).astype(BF16)


def final_kernel(ids, present, pieces, *refs):
    blocks = refs[:8]
    density, php, pt, arrived, hp, sem, sems = refs[8:]
    copies = row_copies(ids, blocks, hp, sems)
    panels = pltpu.make_async_copy(pieces, arrived, sem)
    for copy in [panels] + copies:
        copy.start()
    panels.wait()

    def place(c, _):
        for r in range(ROWS):
            s = c * ROWS + r
            here = pl.ds(pl.multiple_of(s * CW, CW), CW)
            for g in range(RT // CT):
                piece = arrived[c, r, g]
                for a in range(g * CT, g * CT + CT):
                    live = present[s * RT + a] > 0
                    pt[here, pl.ds(a * TILE, TILE)] = jnp.where(live, piece, jnp.zeros_like(piece))
        return 0

    lax.fori_loop(0, COLS, place, 0)
    for copy in copies:
        copy.wait()
    php[...] = lax.dot_general(
        pt[...], hp[...], (((0,), (0,)), ((), ())), preferred_element_type=F32
    )
    mine = pt[pl.ds(pl.multiple_of(ids[1] * WIDTH, WIDTH), WIDTH), :]
    density[...] = mine.T


def from_ring(x, axis):
    return [x] + [lax.ppermute(x, axis, [((i + k) % 4, i) for i in range(4)]) for k in range(1, 4)]


def swapped(x):
    return lax.ppermute(x, "core", [(0, 1), (1, 0)])


def per_device(hamiltonian, pattern, tile_lists, orders, shift):
    row = lax.axis_index(ROW)
    col = lax.axis_index(COL)
    ids = jnp.stack([row, col]).astype(jnp.int32)
    lists = tile_lists.reshape(-1)
    smem = pl.BlockSpec(memory_space=pltpu.SMEM)
    vmem = pl.BlockSpec(memory_space=pltpu.VMEM)
    hbm = pl.BlockSpec(memory_space=pl.ANY)
    flat_pattern = pattern.reshape(-1)
    half = RT * TILE // 2
    ahead = from_ring(hamiltonian[:half], "c1")
    across = from_ring(hamiltonian[half:], "c0")
    strip = from_ring(hamiltonian, "z")
    strip = strip + [swapped(x) for x in strip]
    ahead = from_ring(jnp.stack(ahead), "c0")
    across = from_ring(jnp.stack(across), "c1")
    packed, first = pl.pallas_call(
        pack_kernel,
        out_shape=(
            jax.ShapeDtypeStruct((COLS, 4, TILE, TILE), BF16),
            jax.ShapeDtypeStruct((MAXT, TILE, TILE), BF16),
        ),
        in_specs=[smem, smem, smem] + [hbm] * 8,
        out_specs=(vmem, vmem),
        scratch_shapes=[pltpu.VMEM((NB * TILE, WIDTH), BF16), pltpu.SemaphoreType.DMA((2, 4))],
        name="pack",
    )(ids, lists, orders, *strip)
    packed, ahead, across = lax.optimization_barrier((packed, ahead, across))
    tiles = lax.all_to_all(packed, COL, 0, 0, tiled=True)
    panel = pl.pallas_call(
        solve_kernel,
        out_shape=jax.ShapeDtypeStruct((MAXT, CW, TILE), BF16),
        in_specs=[smem] * 5 + [vmem, vmem],
        out_specs=vmem,
        scratch_shapes=[
            pltpu.VMEM((N, N), BF16),
            pltpu.VMEM((N, N), BF16),
            pltpu.VMEM((N, N), BF16),
            pltpu.VMEM((TILE, N), F32),
        ],
        name="solve",
    )(ids, lists, orders, flat_pattern, shift, tiles, first)
    panels = lax.all_gather(panel, ROW, axis=0, tiled=False)
    spread = pl.pallas_call(
        spread_kernel,
        out_shape=jax.ShapeDtypeStruct((COLS, ROWS, RT // CT, CW, TILE), BF16),
        in_specs=[smem] * 3 + [vmem],
        out_specs=vmem,
        scratch_shapes=[pltpu.VMEM((ROWS, RT // CT, CW, TILE), BF16)],
        name="spread",
    )(ids, lists, orders, panels)
    arrived = lax.all_to_all(spread, COL, 0, 0, tiled=True)
    hp = pl.pallas_call(
        hp_kernel,
        out_shape=jax.ShapeDtypeStruct((RT * TILE, WIDTH), BF16),
        in_specs=[smem] * 4 + [hbm] * 8 + [vmem],
        out_specs=vmem,
        scratch_shapes=[
            pltpu.VMEM((WIDTH, NB * TILE), BF16),
            pltpu.VMEM((RT * TILE, NB * TILE), BF16),
            pltpu.SemaphoreType.DMA((2, 4, 4)),
        ],
        name="hp",
    )(ids, lists, orders, flat_pattern, *ahead, *across, panels)
    ours = from_ring(hp, "z")
    theirs = [swapped(x) for x in ours]
    own = row * RT + jnp.arange(RT, dtype=jnp.int32)
    live = jnp.arange(MAXT, dtype=jnp.int32)[None, :] < orders[:, None]
    present = jnp.any((tile_lists[:, None, :] == own[None, :, None]) & live[:, None, :], axis=2)
    density, php = pl.pallas_call(
        final_kernel,
        out_shape=(
            jax.ShapeDtypeStruct((RT * TILE, WIDTH), BF16),
            jax.ShapeDtypeStruct((RT * TILE, WIDTH), F32),
        ),
        in_specs=[smem, smem] + [hbm] * 9,
        out_specs=(vmem, vmem),
        scratch_shapes=[
            pltpu.VMEM((NB * TILE, RT * TILE), BF16),
            pltpu.VMEM((COLS, ROWS, RT // CT, CW, TILE), BF16),
            pltpu.VMEM((NB * TILE, WIDTH), BF16),
            pltpu.SemaphoreType.DMA,
            pltpu.SemaphoreType.DMA((2, 4)),
        ],
        name="final",
    )(ids, present.astype(jnp.int32).reshape(-1), arrived, *ours, *theirs)
    return density, php


def solution(mesh):
    fine = Mesh(mesh.devices.reshape(4, 2, 4, 4), ("z", "core", "c0", "c1"))
    split = P(ROW, COL)
    return jax.shard_map(
        per_device,
        mesh=fine,
        in_specs=(split, P(), P(), P(), P()),
        out_specs=(split, split),
        check_vma=False,
    )
```

```python
import jax
import jax.numpy as jnp
from jax import lax
from jax.experimental import pallas as pl
from jax.experimental.pallas import tpu as pltpu
from jax.sharding import Mesh
from jax.sharding import PartitionSpec as P

TILE = 128
MAXT = 8
NB = 32
ROWS = 8
COLS = 16
CW = 32
N = MAXT * TILE
RT = NB // ROWS
CT = NB // COLS
WIDTH = CT * TILE
ROW = ("z", "core")
COL = ("c0", "c1")
F32 = jnp.float32
BF16 = jnp.bfloat16


def kept(pattern, a, b):
    return (pattern[a * NB + b] > 0) | (a == b)


def ring_owner(ids, k, part):
    return (ids[0] // 2 + k) % 4 * 2 + (ids[0] + part) % 2


def row_copies(ids, blocks, whole, sems):
    copies = []
    for part in range(2):
        for k in range(4):
            rows = pl.ds(pl.multiple_of(ring_owner(ids, k, part) * RT * TILE, RT * TILE), RT * TILE)
            copies.append(
                pltpu.make_async_copy(blocks[part * 4 + k], whole.at[rows, :], sems.at[part, k])
            )
    return copies


def cyclic(j, k):
    return 1 + (j - 1 + k) % (MAXT - 1)


def pack_kernel(ids, lists, orders, *refs):
    blocks, (out, first, strip, sems) = refs[:8], refs[8:]
    copies = row_copies(ids, blocks, strip, sems)
    for copy in copies:
        copy.start()
    for copy in copies:
        copy.wait()

    def tile(a, lanes):
        return strip[pl.ds(pl.multiple_of(a * TILE, TILE), TILE), lanes]

    own = (ids[1] * ROWS + ids[0]) * MAXT
    lanes = pl.ds(pl.multiple_of(lists[own] % CT * TILE, TILE), TILE)
    for i in range(MAXT):
        first[i] = tile(lists[own + i], lanes)

    def one(c, _):
        s = c * ROWS + ids[0]
        for j in range(1, MAXT):
            b = lists[s * MAXT + j]

            @pl.when((b // CT == ids[1]) & (j < orders[s]))
            def _():
                lanes = pl.ds(pl.multiple_of(b % CT * TILE, TILE), TILE)
                for k in range(4):
                    out[c, k] = tile(lists[s * MAXT + cyclic(j, k)], lanes)

        return 0

    lax.fori_loop(0, COLS, one, 0)


def solve_kernel(ids, lists, orders, pattern, shift, tiles, first, panel, x, f, y, d):
    s = ids[1] * ROWS + ids[0]
    order = orders[s]
    potential = shift[0]
    names = [lists[s * MAXT + j] for j in range(MAXT)]
    rows = lax.broadcasted_iota(jnp.int32, (TILE, TILE), 0)
    cols = lax.broadcasted_iota(jnp.int32, (TILE, TILE), 1)
    eye = jnp.where(rows == cols, 1.0, 0.0).astype(F32)

    def put(i, j, tile):
        y[pl.ds(i * TILE, TILE), pl.ds(j * TILE, TILE)] = tile

    for i in range(MAXT):
        put(i, 0, first[i])
        if i:
            put(0, i, first[i].T)
            for k in range(4):
                tile = tiles[names[i] // CT, k]
                put(cyclic(i, k), i, tile)
                if k:
                    put(i, cyclic(i, k), tile.T)

    def shifted(i, j):
        both = kept(pattern, names[i], names[j]) & (i < order) & (j < order)
        tile = y[pl.ds(i * TILE, TILE), pl.ds(j * TILE, TILE)].astype(F32)
        tile = jnp.where(both, tile, 0.0)
        if i == j:
            tile = tile - jnp.where(i < order, potential, 0.0) * eye
        return tile

    largest = jnp.zeros((), F32)
    for i in range(MAXT):
        total = jnp.zeros((TILE, TILE), F32)
        for j in range(MAXT):
            tile = shifted(i, j)
            total = total + tile * tile
        largest = jnp.maximum(largest, jnp.max(jnp.sum(total, axis=1)))
    root = jnp.sqrt(jnp.full((8, TILE), largest + 1e-06, F32))
    inverse = (1.0 / (jnp.abs(potential) + 2.0 * root))[0:1, :]
    for i in range(MAXT):
        for j in range(MAXT):
            x[pl.ds(i * TILE, TILE), pl.ds(j * TILE, TILE)] = (shifted(i, j) * inverse).astype(BF16)

    band = 512
    brow = lax.broadcasted_iota(jnp.int32, (band, N), 0)
    bcol = lax.broadcasted_iota(jnp.int32, (band, N), 1)

    def step(source, target):
        def square(b, _):
            here = pl.ds(pl.multiple_of(b * band, band), band)
            q = jnp.dot(source[here, :], source[...], preferred_element_type=F32)
            diag = jnp.where(brow + b * band == bcol, 1.5, 0.0)
            f[here, :] = (diag - 0.5 * q).astype(BF16)
            return 0

        def apply(b, _):
            here = pl.ds(pl.multiple_of(b * band, band), band)
            target[here, :] = jnp.dot(
                source[here, :], f[...], preferred_element_type=F32
            ).astype(BF16)
            return 0

        lax.fori_loop(0, N // band, square, 0)
        lax.fori_loop(0, N // band, apply, 0)

    step(x, y)
    step(y, x)
    head = pl.ds(0, TILE)
    prow = lax.broadcasted_iota(jnp.int32, (N, TILE), 0)
    pcol = lax.broadcasted_iota(jnp.int32, (N, TILE), 1)
    q = jnp.dot(x[...], x[:, head], preferred_element_type=F32)
    f[:, head] = (jnp.where(prow == pcol, 1.5, 0.0) - 0.5 * q).astype(BF16)
    z = jnp.dot(x[...], f[:, head], preferred_element_type=F32)
    dens = jnp.where(prow == pcol, 0.5, 0.0) - 0.5 * z
    for i in range(MAXT):
        d[:, pl.ds(i * TILE, TILE)] = dens[i * TILE : (i + 1) * TILE, :].T
    offset = pl.multiple_of(s % (TILE // CW) * CW, CW)
    for i in range(MAXT):
        panel[i] = d[pl.ds(offset, CW), pl.ds(i * TILE, TILE)].astype(BF16)


def spread_kernel(ids, lists, orders, panels, out, mine):
    mine[...] = jnp.zeros_like(mine)
    for k in range(ROWS):
        s = ids[1] * ROWS + k
        for i in range(MAXT):
            group = lists[s * MAXT + i] // CT

            @pl.when((i < orders[s]) & (group // (RT // CT) == ids[0]))
            def _():
                mine[k, group % (RT // CT)] = panels[k, i]

    def one(c, _):
        out[c] = mine[...]
        return 0

    lax.fori_loop(0, COLS, one, 0)


def hp_kernel(ids, lists, orders, pattern, a0, a1, a2, a3, b0, b1, b2, b3, panels, hp, pt, wide, sems):
    half = RT * TILE // 2
    c0 = ids[1] // 4
    c1 = ids[1] % 4
    copies = []
    for k in range(4):
        for m in range(4):
            first = (c0 + k) % 4 * 4 + (c1 + m) % 4
            second = (c0 + m) % 4 * 4 + (c1 + k) % 4
            for part, ref, col in ((0, (a0, a1, a2, a3)[k], first), (1, (b0, b1, b2, b3)[k], second)):
                lanes = pl.ds(pl.multiple_of(col * WIDTH, WIDTH), WIDTH)
                copies.append(
                    pltpu.make_async_copy(
                        ref.at[m], wide.at[pl.ds(part * half, half), lanes], sems.at[part, k, m]
                    )
                )
    for copy in copies:
        copy.start()
    pt[...] = jnp.zeros_like(pt)
    for k in range(ROWS):
        s = ids[1] * ROWS + k
        for i in range(MAXT):

            @pl.when(i < orders[s])
            def _():
                where = pl.multiple_of(lists[s * MAXT + i] * TILE, TILE)
                pt[pl.ds(k * CW, CW), pl.ds(where, TILE)] = panels[k, i]

    for copy in copies:
        copy.wait()

    def clear(b, _):
        lanes = pl.ds(pl.multiple_of(b * TILE, TILE), TILE)
        for a in range(RT):

            @pl.when(jnp.logical_not(kept(pattern, ids[0] * RT + a, b)))
            def _():
                wide[pl.ds(a * TILE, TILE), lanes] = jnp.zeros((TILE, TILE), BF16)

        return 0

    lax.fori_loop(0, NB, clear, 0)
    hp[...] = lax.dot_general(
        wide[...], pt[...], (((1,), (1,)), ((), ())), preferred_element_type=F32
    ).astype(BF16)


def final_kernel(ids, present, pieces, *refs):
    blocks = refs[:8]
    density, php, pt, arrived, hp, sem, sems = refs[8:]
    copies = row_copies(ids, blocks, hp, sems)
    panels = pltpu.make_async_copy(pieces, arrived, sem)
    for copy in [panels] + copies:
        copy.start()
    panels.wait()

    def place(c, _):
        for r in range(ROWS):
            s = c * ROWS + r
            here = pl.ds(pl.multiple_of(s * CW, CW), CW)
            for g in range(RT // CT):
                piece = arrived[c, r, g]
                for a in range(g * CT, g * CT + CT):
                    live = present[s * RT + a] > 0
                    pt[here, pl.ds(a * TILE, TILE)] = jnp.where(live, piece, jnp.zeros_like(piece))
        return 0

    lax.fori_loop(0, COLS, place, 0)
    for copy in copies:
        copy.wait()
    php[...] = lax.dot_general(
        pt[...], hp[...], (((0,), (0,)), ((), ())), preferred_element_type=F32
    )
    mine = pt[pl.ds(pl.multiple_of(ids[1] * WIDTH, WIDTH), WIDTH), :]
    density[...] = mine.T


def from_ring(x, axis):
    return [x] + [lax.ppermute(x, axis, [((i + k) % 4, i) for i in range(4)]) for k in range(1, 4)]


def swapped(x):
    return lax.ppermute(x, "core", [(0, 1), (1, 0)])


def steps(hamiltonian, pattern, tile_lists, orders, shift):
    row = lax.axis_index(ROW)
    col = lax.axis_index(COL)
    ids = jnp.stack([row, col]).astype(jnp.int32)
    lists = tile_lists.reshape(-1)
    smem = pl.BlockSpec(memory_space=pltpu.SMEM)
    vmem = pl.BlockSpec(memory_space=pltpu.VMEM)
    hbm = pl.BlockSpec(memory_space=pl.ANY)
    flat_pattern = pattern.reshape(-1)
    half = RT * TILE // 2
    strip = from_ring(hamiltonian, "z")
    ahead = from_ring(hamiltonian[:half], "c1")
    across = from_ring(hamiltonian[half:], "c0")
    strip = strip + [swapped(x) for x in strip]
    packed, first = pl.pallas_call(
        pack_kernel,
        out_shape=(
            jax.ShapeDtypeStruct((COLS, 4, TILE, TILE), BF16),
            jax.ShapeDtypeStruct((MAXT, TILE, TILE), BF16),
        ),
        in_specs=[smem, smem, smem] + [hbm] * 8,
        out_specs=(vmem, vmem),
        scratch_shapes=[pltpu.VMEM((NB * TILE, WIDTH), BF16), pltpu.SemaphoreType.DMA((2, 4))],
        name="pack",
    )(ids, lists, orders, *strip)
    packed, ahead, across = lax.optimization_barrier((packed, ahead, across))
    tiles = lax.all_to_all(packed, COL, 0, 0, tiled=True)
    ahead = from_ring(jnp.stack(ahead), "c0")
    across = from_ring(jnp.stack(across), "c1")
    panel = pl.pallas_call(
        solve_kernel,
        out_shape=jax.ShapeDtypeStruct((MAXT, CW, TILE), BF16),
        in_specs=[smem] * 5 + [vmem, vmem],
        out_specs=vmem,
        scratch_shapes=[
            pltpu.VMEM((N, N), BF16),
            pltpu.VMEM((N, N), BF16),
            pltpu.VMEM((N, N), BF16),
            pltpu.VMEM((TILE, N), F32),
        ],
        name="solve",
    )(ids, lists, orders, flat_pattern, shift, tiles, first)
    panels = lax.all_gather(panel, ROW, axis=0, tiled=False)
    spread = pl.pallas_call(
        spread_kernel,
        out_shape=jax.ShapeDtypeStruct((COLS, ROWS, RT // CT, CW, TILE), BF16),
        in_specs=[smem] * 3 + [vmem],
        out_specs=vmem,
        scratch_shapes=[pltpu.VMEM((ROWS, RT // CT, CW, TILE), BF16)],
        name="spread",
    )(ids, lists, orders, panels)
    arrived = lax.all_to_all(spread, COL, 0, 0, tiled=True)
    hp = pl.pallas_call(
        hp_kernel,
        out_shape=jax.ShapeDtypeStruct((RT * TILE, WIDTH), BF16),
        in_specs=[smem] * 4 + [hbm] * 8 + [vmem],
        out_specs=vmem,
        scratch_shapes=[
            pltpu.VMEM((WIDTH, NB * TILE), BF16),
            pltpu.VMEM((RT * TILE, NB * TILE), BF16),
            pltpu.SemaphoreType.DMA((2, 4, 4)),
        ],
        name="hp",
    )(ids, lists, orders, flat_pattern, *ahead, *across, panels)
    ours = from_ring(hp, "z")
    theirs = [swapped(x) for x in ours]
    own = row * RT + jnp.arange(RT, dtype=jnp.int32)
    live = jnp.arange(MAXT, dtype=jnp.int32)[None, :] < orders[:, None]
    present = jnp.any((tile_lists[:, None, :] == own[None, :, None]) & live[:, None, :], axis=2)
    density, php = pl.pallas_call(
        final_kernel,
        out_shape=(
            jax.ShapeDtypeStruct((RT * TILE, WIDTH), BF16),
            jax.ShapeDtypeStruct((RT * TILE, WIDTH), F32),
        ),
        in_specs=[smem, smem] + [hbm] * 9,
        out_specs=(vmem, vmem),
        scratch_shapes=[
            pltpu.VMEM((NB * TILE, RT * TILE), BF16),
            pltpu.VMEM((COLS, ROWS, RT // CT, CW, TILE), BF16),
            pltpu.VMEM((NB * TILE, WIDTH), BF16),
            pltpu.SemaphoreType.DMA,
            pltpu.SemaphoreType.DMA((2, 4)),
        ],
        name="final",
    )(ids, present.astype(jnp.int32).reshape(-1), arrived, *ours, *theirs)
    return density, php


def solution(mesh):
    fine = Mesh(mesh.devices.reshape(4, 2, 4, 4), ("z", "core", "c0", "c1"))
    split = P(ROW, COL)
    return jax.shard_map(
        steps,
        mesh=fine,
        in_specs=(split, P(), P(), P(), P()),
        out_specs=(split, split),
        check_vma=False,
    )
```

```python
import jax
import jax.numpy as jnp
from jax import lax
from jax.experimental import pallas as pl
from jax.experimental.pallas import tpu as pltpu
from jax.sharding import Mesh
from jax.sharding import PartitionSpec as P

TILE = 128
MAXT = 8
NB = 32
ROWS = 8
COLS = 16
CW = 32
N = MAXT * TILE
RT = NB // ROWS
CT = NB // COLS
WIDTH = CT * TILE
ROW = ("z", "core")
COL = ("c0", "c1")
F32 = jnp.float32
BF16 = jnp.bfloat16


def kept(pattern, a, b):
    return (pattern[a * NB + b] > 0) | (a == b)


def ring_owner(ids, k, part):
    return (ids[0] // 2 + k) % 4 * 2 + (ids[0] + part) % 2


def join_rows(ids, blocks, whole):
    for part in range(2):
        for k in range(4):
            start = pl.multiple_of(ring_owner(ids, k, part) * RT * TILE, RT * TILE)
            whole[pl.ds(start, RT * TILE), :] = blocks[part * 4 + k][...]


def cyclic(j, k):
    return 1 + (j - 1 + k) % (MAXT - 1)


def pack_kernel(ids, lists, orders, *refs):
    blocks, (out, first, strip, sems) = refs[:8], refs[8:]
    join_rows(ids, blocks, strip)

    def send(c, k, row, lanes):
        start = pl.multiple_of(row * TILE, TILE)
        lanes = pl.ds(pl.multiple_of(lanes * TILE, TILE), TILE)
        return pltpu.make_async_copy(
            strip.at[pl.ds(start, TILE), lanes], out.at[c, k], sems.at[c, k]
        )

    def one(c, _):
        s = c * ROWS + ids[0]
        which = jnp.int32(1)
        for j in range(2, MAXT):
            hit = (lists[s * MAXT + j] // CT == ids[1]) & (j < orders[s])
            which = jnp.where(hit, j, which)
        side = lists[s * MAXT + which] % CT
        for k in range(4):
            send(c, k, lists[s * MAXT + cyclic(which, k)], side).start()
        return 0

    lax.fori_loop(0, COLS, one, 0)

    def tile(a, lanes):
        return strip[pl.ds(pl.multiple_of(a * TILE, TILE), TILE), lanes]

    own = (ids[1] * ROWS + ids[0]) * MAXT
    lanes = pl.ds(pl.multiple_of(lists[own] % CT * TILE, TILE), TILE)
    for i in range(MAXT):
        first[i] = tile(lists[own + i], lanes)

    def done(c, _):
        for k in range(4):
            send(c, k, 0, 0).wait()
        return 0

    lax.fori_loop(0, COLS, done, 0)


def solve_kernel(ids, lists, orders, pattern, shift, tiles, first, panel, x, f, y, d):
    s = ids[1] * ROWS + ids[0]
    order = orders[s]
    potential = shift[0]
    names = [lists[s * MAXT + j] for j in range(MAXT)]
    rows = lax.broadcasted_iota(jnp.int32, (TILE, TILE), 0)
    cols = lax.broadcasted_iota(jnp.int32, (TILE, TILE), 1)
    eye = jnp.where(rows == cols, 1.0, 0.0).astype(F32)

    def put(i, j, tile):
        y[pl.ds(i * TILE, TILE), pl.ds(j * TILE, TILE)] = tile

    def masked(i, j, tile):
        both = kept(pattern, names[i], names[j]) & (i < order) & (j < order)
        return jnp.where(both, tile, jnp.zeros_like(tile))

    for i in range(MAXT):
        tile = masked(i, 0, first[i])
        put(i, 0, tile)
        if i:
            put(0, i, tile.T)
            for k in range(4):
                tile = masked(cyclic(i, k), i, tiles[names[i] // CT, k])
                put(cyclic(i, k), i, tile)
                if k:
                    put(i, cyclic(i, k), tile.T)

    def shifted(i, j):
        tile = y[pl.ds(i * TILE, TILE), pl.ds(j * TILE, TILE)].astype(F32)
        if i == j:
            tile = tile - jnp.where(i < order, potential, 0.0) * eye
        return tile

    largest = jnp.zeros((), F32)
    for i in range(MAXT):
        total = jnp.zeros((TILE, TILE), F32)
        for j in range(MAXT):
            tile = shifted(i, j)
            total = total + tile * tile
        largest = jnp.maximum(largest, jnp.max(jnp.sum(total, axis=1)))
    root = jnp.sqrt(jnp.full((8, TILE), largest + 1e-06, F32))
    inverse = (1.0 / (jnp.abs(potential) + 2.0 * root))[0:1, :]
    for i in range(MAXT):
        for j in range(MAXT):
            x[pl.ds(i * TILE, TILE), pl.ds(j * TILE, TILE)] = (shifted(i, j) * inverse).astype(BF16)

    band = 512
    brow = lax.broadcasted_iota(jnp.int32, (band, N), 0)
    bcol = lax.broadcasted_iota(jnp.int32, (band, N), 1)

    def step(source, target):
        def square(b, _):
            here = pl.ds(pl.multiple_of(b * band, band), band)
            q = jnp.dot(source[here, :], source[...], preferred_element_type=F32)
            diag = jnp.where(brow + b * band == bcol, 1.5, 0.0)
            f[here, :] = (diag - 0.5 * q).astype(BF16)
            return 0

        def apply(b, _):
            here = pl.ds(pl.multiple_of(b * band, band), band)
            target[here, :] = jnp.dot(
                source[here, :], f[...], preferred_element_type=F32
            ).astype(BF16)
            return 0

        lax.fori_loop(0, N // band, square, 0)
        lax.fori_loop(0, N // band, apply, 0)

    step(x, y)
    step(y, x)
    head = pl.ds(0, TILE)
    prow = lax.broadcasted_iota(jnp.int32, (N, TILE), 0)
    pcol = lax.broadcasted_iota(jnp.int32, (N, TILE), 1)
    q = jnp.dot(x[...], x[:, head], preferred_element_type=F32)
    f[:, head] = (jnp.where(prow == pcol, 1.5, 0.0) - 0.5 * q).astype(BF16)
    z = jnp.dot(x[...], f[:, head], preferred_element_type=F32)
    dens = jnp.where(prow == pcol, 0.5, 0.0) - 0.5 * z
    for i in range(MAXT):
        d[:, pl.ds(i * TILE, TILE)] = dens[i * TILE : (i + 1) * TILE, :].T
    offset = pl.multiple_of(s % (TILE // CW) * CW, CW)
    for i in range(MAXT):
        panel[i] = d[pl.ds(offset, CW), pl.ds(i * TILE, TILE)].astype(BF16)


def spread_kernel(ids, lists, orders, panels, out, mine, sems):
    mine[...] = jnp.zeros_like(mine)
    for k in range(ROWS):
        s = ids[1] * ROWS + k
        for i in range(MAXT):
            group = lists[s * MAXT + i] // CT

            @pl.when((i < orders[s]) & (group // (RT // CT) == ids[0]))
            def _():
                mine[k, group % (RT // CT)] = panels[k, i]

    copies = [pltpu.make_async_copy(mine, out.at[c], sems.at[c]) for c in range(COLS)]
    for copy in copies:
        copy.start()
    for copy in copies:
        copy.wait()


def hp_kernel(ids, lists, orders, pattern, a0, a1, a2, a3, b0, b1, b2, b3, panels, hp, pt, wide):
    c0 = ids[1] // 4
    c1 = ids[1] % 4
    for k in range(4):
        for m in range(4):
            first = (c0 + k) % 4 * 4 + (c1 + m) % 4
            second = (c0 + m) % 4 * 4 + (c1 + k) % 4
            for part, ref, col in ((0, (a0, a1, a2, a3)[k], first), (1, (b0, b1, b2, b3)[k], second)):
                for i in range(RT // 2):
                    for j in range(CT):
                        a = part * (RT // 2) + i
                        b = col * CT + j
                        tile = ref[m, pl.ds(i * TILE, TILE), pl.ds(j * TILE, TILE)]
                        live = kept(pattern, ids[0] * RT + a, b)
                        wide[
                            pl.ds(a * TILE, TILE), pl.ds(pl.multiple_of(b * TILE, TILE), TILE)
                        ] = jnp.where(live, tile, jnp.zeros_like(tile))
    pt[...] = jnp.zeros_like(pt)
    for k in range(ROWS):
        s = ids[1] * ROWS + k
        for i in range(MAXT):

            @pl.when(i < orders[s])
            def _():
                where = pl.multiple_of(lists[s * MAXT + i] * TILE, TILE)
                pt[pl.ds(k * CW, CW), pl.ds(where, TILE)] = panels[k, i]

    hp[...] = lax.dot_general(
        wide[...], pt[...], (((1,), (1,)), ((), ())), preferred_element_type=F32
    ).astype(BF16)


def final_kernel(ids, present, pieces, *refs):
    blocks = refs[:8]
    density, php, pt, hp = refs[8:]
    join_rows(ids, blocks, hp)

    def place(c, _):
        for r in range(ROWS):
            s = c * ROWS + r
            here = pl.ds(pl.multiple_of(s * CW, CW), CW)
            for g in range(RT // CT):
                piece = pieces[c, r, g]
                for a in range(g * CT, g * CT + CT):
                    live = present[s * RT + a] > 0
                    pt[here, pl.ds(a * TILE, TILE)] = jnp.where(live, piece, jnp.zeros_like(piece))
        return 0

    lax.fori_loop(0, COLS, place, 0)
    php[...] = lax.dot_general(
        pt[...], hp[...], (((0,), (0,)), ((), ())), preferred_element_type=F32
    )
    mine = pt[pl.ds(pl.multiple_of(ids[1] * WIDTH, WIDTH), WIDTH), :]
    density[...] = mine.T


def from_ring(x, axis):
    return [x] + [lax.ppermute(x, axis, [((i + k) % 4, i) for i in range(4)]) for k in range(1, 4)]


def swapped(x):
    return lax.ppermute(x, "core", [(0, 1), (1, 0)])


SMEM = pl.BlockSpec(memory_space=pltpu.SMEM)
LOCAL = pl.BlockSpec(memory_space=pltpu.VMEM)
FAR = pl.BlockSpec(memory_space=pl.ANY)


def call(kernel, outs, scratch, small, large, specs=LOCAL):
    return pl.pallas_call(
        kernel,
        out_shape=outs,
        in_specs=[SMEM] * len(small) + [LOCAL] * len(large),
        out_specs=specs,
        scratch_shapes=scratch,
        compiler_params=pltpu.CompilerParams(vmem_limit_bytes=24 << 20),
    )(*small, *[pltpu.with_memory_space_constraint(x, pltpu.VMEM) for x in large])


def call_solve(ids, lists, orders, pattern, shift, tiles, first):
    return call(
        solve_kernel,
        pltpu.VMEM((MAXT, CW, TILE), BF16),
        [pltpu.VMEM((N, N), BF16)] * 3 + [pltpu.VMEM((TILE, N), F32)],
        (ids, lists, orders, pattern, shift),
        (tiles, first),
    )


def steps(hamiltonian, pattern, tile_lists, orders, shift):
    row = lax.axis_index(ROW)
    col = lax.axis_index(COL)
    ids = jnp.stack([row, col]).astype(jnp.int32)
    lists = tile_lists.reshape(-1)
    flat_pattern = pattern.reshape(-1)
    half = RT * TILE // 2
    strip = from_ring(hamiltonian, "z")
    ahead = from_ring(hamiltonian[:half], "c1")
    across = from_ring(hamiltonian[half:], "c0")
    strip = strip + [swapped(x) for x in strip]
    packed, first = call(
        pack_kernel,
        (pltpu.HBM((COLS, 4, TILE, TILE), BF16), pltpu.VMEM((MAXT, TILE, TILE), BF16)),
        [pltpu.VMEM((NB * TILE, WIDTH), BF16), pltpu.SemaphoreType.DMA((COLS, 4))],
        (ids, lists, orders),
        strip,
        (FAR, LOCAL),
    )
    packed, ahead, across = lax.optimization_barrier((packed, ahead, across))
    tiles = lax.all_to_all(packed, COL, 0, 0, tiled=True)
    ahead = from_ring(jnp.stack(ahead), "c0")
    across = from_ring(jnp.stack(across), "c1")
    panel = call_solve(ids, lists, orders, flat_pattern, shift, tiles, first)
    panels = lax.all_gather(panel, ROW, axis=0, tiled=False)
    spread = call(
        spread_kernel,
        pltpu.HBM((COLS, ROWS, RT // CT, CW, TILE), BF16),
        [pltpu.VMEM((ROWS, RT // CT, CW, TILE), BF16), pltpu.SemaphoreType.DMA((COLS,))],
        (ids, lists, orders),
        (panels,),
        FAR,
    )
    arrived = lax.all_to_all(spread, COL, 0, 0, tiled=True)
    hp = call(
        hp_kernel,
        pltpu.VMEM((RT * TILE, WIDTH), BF16),
        [pltpu.VMEM((WIDTH, NB * TILE), BF16), pltpu.VMEM((RT * TILE, NB * TILE), BF16)],
        (ids, lists, orders, flat_pattern),
        (*ahead, *across, panels),
    )
    ours = from_ring(hp, "z")
    theirs = [swapped(x) for x in ours]
    own = row * RT + jnp.arange(RT, dtype=jnp.int32)
    live = jnp.arange(MAXT, dtype=jnp.int32)[None, :] < orders[:, None]
    present = jnp.any((tile_lists[:, None, :] == own[None, :, None]) & live[:, None, :], axis=2)
    density, php = call(
        final_kernel,
        (
            jax.ShapeDtypeStruct((RT * TILE, WIDTH), BF16),
            jax.ShapeDtypeStruct((RT * TILE, WIDTH), F32),
        ),
        [pltpu.VMEM((NB * TILE, RT * TILE), BF16), pltpu.VMEM((NB * TILE, WIDTH), BF16)],
        (ids, present.astype(jnp.int32).reshape(-1)),
        (arrived, *ours, *theirs),
        (LOCAL, LOCAL),
    )
    return density, php


def solution(mesh):
    fine = Mesh(mesh.devices.reshape(4, 2, 4, 4), ("z", "core", "c0", "c1"))
    split = P(ROW, COL)
    return jax.shard_map(
        steps,
        mesh=fine,
        in_specs=(split, P(), P(), P(), P()),
        out_specs=(split, split),
        check_vma=False,
    )
```

```python
import jax
import jax.numpy as jnp
from jax import lax
from jax.experimental import pallas as pl
from jax.experimental.pallas import tpu as pltpu
from jax.sharding import Mesh
from jax.sharding import PartitionSpec as P

TILE = 128
MAXT = 8
NB = 32
ROWS = 8
COLS = 16
SUBS = 128
CW = 32
N = MAXT * TILE
RT = NB // ROWS
CT = NB // COLS
WIDTH = CT * TILE
ROW = ("z", "core")
COL = ("c0", "c1")
F32 = jnp.float32
BF16 = jnp.bfloat16


class Table:
    def __init__(self, ref):
        self.lists = Part(ref, 0)
        self.orders = Part(ref, SUBS * MAXT)
        self.pattern = Part(ref, SUBS * MAXT + SUBS)
        self.ids = Part(ref, SUBS * MAXT + SUBS + NB * NB)


class Part:
    def __init__(self, ref, base):
        self.ref = ref
        self.base = base

    def __getitem__(self, index):
        return self.ref[self.base + index]


def kept(pattern, a, b):
    return (pattern[a * NB + b] > 0) | (a == b)


def ring_owner(ids, k, part):
    return (ids[0] // 2 + k) % 4 * 2 + (ids[0] + part) % 2


def join_rows(ids, blocks, whole):
    for part in range(2):
        for k in range(4):
            block = blocks[part * 4 + k]
            pieces = block if isinstance(block, tuple) else (block,)
            size = RT * TILE // len(pieces)
            start = ring_owner(ids, k, part) * RT * TILE
            for number, piece in enumerate(pieces):
                whole[pl.ds(pl.multiple_of(start + number * size, size), size), :] = piece[...]


def cyclic(j, k):
    return 1 + (j - 1 + k) % (MAXT - 1)


def pack_kernel(table, *refs):
    table = Table(table)
    ids, lists, orders = table.ids, table.lists, table.orders
    halves, blocks, (out, first, strip, sems) = refs[:2], refs[2:9], refs[9:]
    join_rows(ids, (halves, *blocks), strip)

    def send(c, k, row, lanes):
        start = pl.multiple_of(row * TILE, TILE)
        lanes = pl.ds(pl.multiple_of(lanes * TILE, TILE), TILE)
        return pltpu.make_async_copy(
            strip.at[pl.ds(start, TILE), lanes], out.at[c, k], sems.at[c, k]
        )

    def one(c, _):
        s = c * ROWS + ids[0]
        which = jnp.int32(1)
        for j in range(2, MAXT):
            hit = (lists[s * MAXT + j] // CT == ids[1]) & (j < orders[s])
            which = jnp.where(hit, j, which)
        side = lists[s * MAXT + which] % CT
        for k in range(4):
            send(c, k, lists[s * MAXT + cyclic(which, k)], side).start()
        return 0

    lax.fori_loop(0, COLS, one, 0)

    def tile(a, lanes):
        return strip[pl.ds(pl.multiple_of(a * TILE, TILE), TILE), lanes]

    own = (ids[1] * ROWS + ids[0]) * MAXT
    lanes = pl.ds(pl.multiple_of(lists[own] % CT * TILE, TILE), TILE)
    for i in range(MAXT):
        first[i] = tile(lists[own + i], lanes)

    def done(c, _):
        for k in range(4):
            send(c, k, 0, 0).wait()
        return 0

    lax.fori_loop(0, COLS, done, 0)


def solve_kernel(table, shift, tiles, first, panel, x, f, y):
    table = Table(table)
    ids, lists, pattern = table.ids, table.lists, table.pattern
    s = ids[1] * ROWS + ids[0]
    order = table.orders[s]
    potential = shift[0]
    names = [lists[s * MAXT + j] for j in range(MAXT)]
    rows = lax.broadcasted_iota(jnp.int32, (TILE, TILE), 0)
    cols = lax.broadcasted_iota(jnp.int32, (TILE, TILE), 1)
    eye = jnp.where(rows == cols, 1.0, 0.0).astype(F32)

    def put(i, j, tile):
        y[pl.ds(i * TILE, TILE), pl.ds(j * TILE, TILE)] = tile

    def masked(i, j, tile):
        both = kept(pattern, names[i], names[j]) & (i < order) & (j < order)
        return jnp.where(both, tile, jnp.zeros_like(tile))

    for i in range(MAXT):
        tile = masked(i, 0, first[i])
        put(i, 0, tile)
        if i:
            put(0, i, tile.T)
            for k in range(4):
                tile = masked(cyclic(i, k), i, tiles[names[i] // CT, k])
                put(cyclic(i, k), i, tile)
                if k:
                    put(i, cyclic(i, k), tile.T)

    def shifted(i, j):
        tile = y[pl.ds(i * TILE, TILE), pl.ds(j * TILE, TILE)].astype(F32)
        if i == j:
            tile = tile - jnp.where(i < order, potential, 0.0) * eye
        return tile

    largest = jnp.zeros((), F32)
    for i in range(MAXT):
        total = jnp.zeros((TILE, TILE), F32)
        for j in range(MAXT):
            tile = shifted(i, j)
            total = total + tile * tile
        largest = jnp.maximum(largest, jnp.max(jnp.sum(total, axis=1)))
    root = jnp.sqrt(jnp.full((8, TILE), largest + 1e-06, F32))
    inverse = (1.0 / (jnp.abs(potential) + 2.0 * root))[0:1, :]
    for i in range(MAXT):
        for j in range(MAXT):
            x[pl.ds(i * TILE, TILE), pl.ds(j * TILE, TILE)] = (shifted(i, j) * inverse).astype(BF16)

    band = 256
    brow = lax.broadcasted_iota(jnp.int32, (band, N), 0)
    bcol = lax.broadcasted_iota(jnp.int32, (band, N), 1)

    def step(source, target):
        blocks = N // band
        for b in range(blocks):
            here = slice(b * band, b * band + band)
            rest = slice(b * band, N)
            q = lax.dot_general(
                source[here, :], source[:, rest], (((1,), (0,)), ((), ())), preferred_element_type=F32
            )
            diag = jnp.where(brow[:, : N - b * band] == bcol[:, : N - b * band], 1.5, 0.0)
            part = (diag - 0.5 * q).astype(BF16)
            f[here, rest] = part
            for c in range(b + 1, blocks):
                f[c * band : c * band + band, here] = part[:, (c - b) * band : (c - b + 1) * band].T
        for b in range(blocks):
            here = slice(b * band, b * band + band)
            rest = slice(b * band, N)
            part = jnp.dot(source[here, :], f[:, rest], preferred_element_type=F32).astype(BF16)
            target[here, rest] = part
            for c in range(b + 1, blocks):
                target[c * band : c * band + band, here] = part[
                    :, (c - b) * band : (c - b + 1) * band
                ].T

    step(x, y)
    step(y, x)
    offset = pl.multiple_of(s % (TILE // CW) * CW, CW)
    prow = lax.broadcasted_iota(jnp.int32, (CW, N), 0) + offset
    pcol = lax.broadcasted_iota(jnp.int32, (CW, N), 1)
    q = jnp.dot(x[pl.ds(offset, CW), :], x[...], preferred_element_type=F32)
    part = (jnp.where(prow == pcol, 1.5, 0.0) - 0.5 * q).astype(BF16)
    z = jnp.dot(part, x[...], preferred_element_type=F32)
    dens = (jnp.where(prow == pcol, 0.5, 0.0) - 0.5 * z).astype(BF16)
    for i in range(MAXT):
        panel[i] = dens[:, i * TILE : (i + 1) * TILE]


def spread_kernel(table, panels, out, mine, sems):
    table = Table(table)
    ids, lists, orders = table.ids, table.lists, table.orders
    mine[...] = jnp.zeros_like(mine)
    for k in range(ROWS):
        s = ids[1] * ROWS + k
        for i in range(MAXT):
            group = lists[s * MAXT + i] // CT

            @pl.when((i < orders[s]) & (group // (RT // CT) == ids[0]))
            def _():
                mine[k, group % (RT // CT)] = panels[k, i]

    copies = [pltpu.make_async_copy(mine, out.at[c], sems.at[c]) for c in range(COLS)]
    for copy in copies:
        copy.start()
    for copy in copies:
        copy.wait()


def hp_kernel(table, a0, a1, a2, a3, b0, b1, b2, b3, panels, hp, pt, wide):
    table = Table(table)
    ids, lists, orders, pattern = table.ids, table.lists, table.orders, table.pattern
    half = RT * TILE // 2
    c0 = ids[1] // 4
    c1 = ids[1] % 4
    for k in range(4):
        for m in range(4):
            first = (c0 + k) % 4 * 4 + (c1 + m) % 4
            second = (c0 + m) % 4 * 4 + (c1 + k) % 4
            for part, ref, col in ((0, (a0, a1, a2, a3)[k], first), (1, (b0, b1, b2, b3)[k], second)):
                for i in range(RT // 2):
                    for j in range(CT):
                        a = part * (RT // 2) + i
                        b = col * CT + j
                        tile = ref[m, pl.ds(i * TILE, TILE), pl.ds(j * TILE, TILE)]
                        live = kept(pattern, ids[0] * RT + a, b)
                        wide[
                            pl.ds(a * TILE, TILE), pl.ds(pl.multiple_of(b * TILE, TILE), TILE)
                        ] = jnp.where(live, tile, jnp.zeros_like(tile))
    pt[...] = jnp.zeros_like(pt)
    for k in range(ROWS):
        s = ids[1] * ROWS + k
        for i in range(MAXT):

            @pl.when(i < orders[s])
            def _():
                where = pl.multiple_of(lists[s * MAXT + i] * TILE, TILE)
                pt[pl.ds(k * CW, CW), pl.ds(where, TILE)] = panels[k, i]

    hp[...] = lax.dot_general(
        wide[...], pt[...], (((1,), (1,)), ((), ())), preferred_element_type=F32
    ).astype(BF16)


def final_kernel(table, present, pieces, *refs):
    blocks = refs[:8]
    density, php, pt, hp = refs[8:]
    ids = Table(table).ids
    join_rows(ids, blocks, hp)

    def place(c, _):
        for r in range(ROWS):
            s = c * ROWS + r
            here = pl.ds(pl.multiple_of(s * CW, CW), CW)
            for g in range(RT // CT):
                piece = pieces[c, r, g]
                for a in range(g * CT, g * CT + CT):
                    live = present[s * RT + a] > 0
                    pt[here, pl.ds(a * TILE, TILE)] = jnp.where(live, piece, jnp.zeros_like(piece))
        return 0

    lax.fori_loop(0, COLS, place, 0)
    php[...] = lax.dot_general(
        pt[...], hp[...], (((0,), (0,)), ((), ())), preferred_element_type=F32
    )
    mine = pt[pl.ds(pl.multiple_of(ids[1] * WIDTH, WIDTH), WIDTH), :]
    density[...] = mine.T


def from_ring(x, axis):
    return [x] + [lax.ppermute(x, axis, [((i + k) % 4, i) for i in range(4)]) for k in range(1, 4)]


def swapped(x):
    return lax.ppermute(x, "core", [(0, 1), (1, 0)])


SMEM = pl.BlockSpec(memory_space=pltpu.SMEM)
LOCAL = pl.BlockSpec(memory_space=pltpu.VMEM)
FAR = pl.BlockSpec(memory_space=pl.ANY)


def call(kernel, outs, scratch, small, large, specs=LOCAL):
    return pl.pallas_call(
        kernel,
        out_shape=outs,
        in_specs=[SMEM] * len(small) + [LOCAL] * len(large),
        out_specs=specs,
        scratch_shapes=scratch,
        compiler_params=pltpu.CompilerParams(vmem_limit_bytes=24 << 20),
    )(*small, *[pltpu.with_memory_space_constraint(x, pltpu.VMEM) for x in large])


def call_solve(table, shift, tiles, first):
    return call(
        solve_kernel,
        pltpu.VMEM((MAXT, CW, TILE), BF16),
        [pltpu.VMEM((N, N), BF16)] * 3,
        (table, shift),
        (tiles, first),
    )


def steps(hamiltonian, pattern, tile_lists, orders, shift):
    row = lax.axis_index(ROW)
    col = lax.axis_index(COL)
    ids = jnp.stack([row, col]).astype(jnp.int32)
    table = jnp.concatenate([tile_lists.reshape(-1), orders, pattern.reshape(-1), ids])
    half = RT * TILE // 2
    top, bottom = hamiltonian[:half], hamiltonian[half:]
    strip = from_ring(hamiltonian, "z")
    ahead = jnp.stack(from_ring(top, "c1"))
    across = jnp.stack(from_ring(bottom, "c0"))
    strip = strip + [swapped(x) for x in strip]
    packed, first = call(
        pack_kernel,
        (pltpu.HBM((COLS, 4, TILE, TILE), BF16), pltpu.VMEM((MAXT, TILE, TILE), BF16)),
        [pltpu.VMEM((NB * TILE, WIDTH), BF16), pltpu.SemaphoreType.DMA((COLS, 4))],
        (table,),
        (top, bottom, *strip[1:]),
        (FAR, LOCAL),
    )
    packed, ahead, across = lax.optimization_barrier((packed, ahead, across))
    tiles = lax.all_to_all(packed, COL, 0, 0, tiled=True)
    ahead = from_ring(ahead, "c0")
    across = from_ring(across, "c1")
    panel = call_solve(table, shift, tiles, first)
    panels = lax.all_gather(panel, ROW, axis=0, tiled=False)
    spread = call(
        spread_kernel,
        pltpu.HBM((COLS, ROWS, RT // CT, CW, TILE), BF16),
        [pltpu.VMEM((ROWS, RT // CT, CW, TILE), BF16), pltpu.SemaphoreType.DMA((COLS,))],
        (table,),
        (panels,),
        FAR,
    )
    arrived = lax.all_to_all(spread, COL, 0, 0, tiled=True)
    hp = call(
        hp_kernel,
        pltpu.VMEM((RT * TILE, WIDTH), BF16),
        [pltpu.VMEM((WIDTH, NB * TILE), BF16), pltpu.VMEM((RT * TILE, NB * TILE), BF16)],
        (table,),
        (*ahead, *across, panels),
    )
    ours = from_ring(hp, "z")
    theirs = [swapped(x) for x in ours]
    own = row * RT + jnp.arange(RT, dtype=jnp.int32)
    live = jnp.arange(MAXT, dtype=jnp.int32)[None, :] < orders[:, None]
    present = jnp.any((tile_lists[:, None, :] == own[None, :, None]) & live[:, None, :], axis=2)
    density, php = call(
        final_kernel,
        (
            jax.ShapeDtypeStruct((RT * TILE, WIDTH), BF16),
            jax.ShapeDtypeStruct((RT * TILE, WIDTH), F32),
        ),
        [pltpu.VMEM((NB * TILE, RT * TILE), BF16), pltpu.VMEM((NB * TILE, WIDTH), BF16)],
        (table, present.astype(jnp.int32).reshape(-1)),
        (arrived, *ours, *theirs),
        (LOCAL, LOCAL),
    )
    return density, php


def solution(mesh):
    fine = Mesh(mesh.devices.reshape(4, 2, 4, 4), ("z", "core", "c0", "c1"))
    split = P(ROW, COL)
    return jax.shard_map(
        steps,
        mesh=fine,
        in_specs=(split, P(), P(), P(), P()),
        out_specs=(split, split),
        check_vma=False,
    )
```

```python
import jax
import jax.numpy as jnp
from jax import lax
from jax.experimental import pallas as pl
from jax.experimental.pallas import tpu as pltpu
from jax.sharding import Mesh
from jax.sharding import PartitionSpec as P

TILE = 128
MAXT = 8
NB = 32
ROWS = 8
COLS = 16
SUBS = 128
CW = 32
PAUSE = 1300
N = MAXT * TILE
RT = NB // ROWS
CT = NB // COLS
WIDTH = CT * TILE
ROW = ("z", "core")
COL = ("c0", "c1")
F32 = jnp.float32
BF16 = jnp.bfloat16


class Table:
    def __init__(self, ref):
        self.lists = Part(ref, 0)
        self.orders = Part(ref, SUBS * MAXT)
        self.pattern = Part(ref, SUBS * MAXT + SUBS)
        self.ids = Part(ref, SUBS * MAXT + SUBS + NB * NB)


class Part:
    def __init__(self, ref, base):
        self.ref = ref
        self.base = base

    def __getitem__(self, index):
        return self.ref[self.base + index]


def kept(pattern, a, b):
    return (pattern[a * NB + b] > 0) | (a == b)


def ring_owner(ids, k, part):
    return (ids[0] // 2 + k) % 4 * 2 + (ids[0] + part) % 2


def join_rows(ids, blocks, whole):
    for part in range(2):
        for k in range(4):
            block = blocks[part * 4 + k]
            pieces = block if isinstance(block, tuple) else (block,)
            size = RT * TILE // len(pieces)
            start = ring_owner(ids, k, part) * RT * TILE
            for number, piece in enumerate(pieces):
                whole[pl.ds(pl.multiple_of(start + number * size, size), size), :] = piece[...]


def cyclic(j, k):
    return 1 + (j - 1 + k) % (MAXT - 1)


def pack_kernel(table, *refs):
    table = Table(table)
    ids, lists, orders = table.ids, table.lists, table.orders
    halves, blocks, (out, first, strip, sems) = refs[:2], refs[2:9], refs[9:]
    join_rows(ids, (halves, *blocks), strip)

    def send(c, k, row, lanes):
        start = pl.multiple_of(row * TILE, TILE)
        lanes = pl.ds(pl.multiple_of(lanes * TILE, TILE), TILE)
        return pltpu.make_async_copy(
            strip.at[pl.ds(start, TILE), lanes], out.at[c, k], sems.at[c, k]
        )

    def one(c, _):
        s = c * ROWS + ids[0]
        which = jnp.int32(1)
        for j in range(2, MAXT):
            hit = (lists[s * MAXT + j] // CT == ids[1]) & (j < orders[s])
            which = jnp.where(hit, j, which)
        side = lists[s * MAXT + which] % CT
        for k in range(4):
            send(c, k, lists[s * MAXT + cyclic(which, k)], side).start()
        return 0

    lax.fori_loop(0, COLS, one, 0)

    own = (ids[1] * ROWS + ids[0]) * MAXT
    side = pl.ds(pl.multiple_of(lists[own] % CT * TILE, TILE), TILE)
    heads = [
        pltpu.make_async_copy(
            strip.at[pl.ds(pl.multiple_of(lists[own + i] * TILE, TILE), TILE), side],
            first.at[i],
            sems.at[COLS + i // 4, i % 4],
        )
        for i in range(MAXT)
    ]
    for copy in heads:
        copy.start()

    def done(c, _):
        for k in range(4):
            send(c, k, 0, 0).wait()
        return 0

    lax.fori_loop(0, COLS, done, 0)
    for copy in heads:
        copy.wait()


def solve_kernel(table, shift, tiles, first, panel, x, f, y):
    table = Table(table)
    ids, lists, pattern = table.ids, table.lists, table.pattern
    s = ids[1] * ROWS + ids[0]
    order = table.orders[s]
    potential = shift[0]
    names = [lists[s * MAXT + j] for j in range(MAXT)]
    rows = lax.broadcasted_iota(jnp.int32, (TILE, TILE), 0)
    cols = lax.broadcasted_iota(jnp.int32, (TILE, TILE), 1)
    eye = jnp.where(rows == cols, 1.0, 0.0).astype(F32)

    def put(i, j, tile):
        y[pl.ds(i * TILE, TILE), pl.ds(j * TILE, TILE)] = tile

    def masked(i, j, tile):
        both = kept(pattern, names[i], names[j]) & (i < order) & (j < order)
        return jnp.where(both, tile, jnp.zeros_like(tile))

    for i in range(MAXT):
        tile = masked(i, 0, first[i])
        put(i, 0, tile)
        if i:
            put(0, i, tile.T)
            for k in range(4):
                tile = masked(cyclic(i, k), i, tiles[names[i] // CT, k])
                put(cyclic(i, k), i, tile)
                if k:
                    put(i, cyclic(i, k), tile.T)

    def shifted(i, j):
        tile = y[pl.ds(i * TILE, TILE), pl.ds(j * TILE, TILE)].astype(F32)
        if i == j:
            tile = tile - jnp.where(i < order, potential, 0.0) * eye
        return tile

    largest = jnp.zeros((), F32)
    for i in range(MAXT):
        total = jnp.zeros((TILE, TILE), F32)
        for j in range(MAXT):
            tile = shifted(i, j)
            total = total + tile * tile
        largest = jnp.maximum(largest, jnp.max(jnp.sum(total, axis=1)))
    root = jnp.sqrt(jnp.full((8, TILE), largest + 1e-06, F32))
    inverse = (1.0 / (jnp.abs(potential) + 2.0 * root))[0:1, :]
    for i in range(MAXT):
        for j in range(MAXT):
            x[pl.ds(i * TILE, TILE), pl.ds(j * TILE, TILE)] = (shifted(i, j) * inverse).astype(BF16)

    band = 256
    brow = lax.broadcasted_iota(jnp.int32, (band, N), 0)
    bcol = lax.broadcasted_iota(jnp.int32, (band, N), 1)

    def step(source, target):
        blocks = N // band
        for b in range(blocks):
            here = slice(b * band, b * band + band)
            rest = slice(b * band, N)
            q = lax.dot_general(
                source[here, :], source[:, rest], (((1,), (0,)), ((), ())), preferred_element_type=F32
            )
            diag = jnp.where(brow[:, : N - b * band] == bcol[:, : N - b * band], 1.5, 0.0)
            part = (diag - 0.5 * q).astype(BF16)
            f[here, rest] = part
            for c in range(b + 1, blocks):
                f[c * band : c * band + band, here] = part[:, (c - b) * band : (c - b + 1) * band].T
        for b in range(blocks):
            here = slice(b * band, b * band + band)
            rest = slice(b * band, N)
            part = jnp.dot(source[here, :], f[:, rest], preferred_element_type=F32).astype(BF16)
            target[here, rest] = part
            for c in range(b + 1, blocks):
                target[c * band : c * band + band, here] = part[
                    :, (c - b) * band : (c - b + 1) * band
                ].T

    step(x, y)
    step(y, x)
    offset = pl.multiple_of(s % (TILE // CW) * CW, CW)
    prow = lax.broadcasted_iota(jnp.int32, (CW, N), 0) + offset
    pcol = lax.broadcasted_iota(jnp.int32, (CW, N), 1)
    q = jnp.dot(x[pl.ds(offset, CW), :], x[...], preferred_element_type=F32)
    part = (jnp.where(prow == pcol, 1.5, 0.0) - 0.5 * q).astype(BF16)
    z = jnp.dot(part, x[...], preferred_element_type=F32)
    dens = (jnp.where(prow == pcol, 0.5, 0.0) - 0.5 * z).astype(BF16)
    for i in range(MAXT):
        panel[i] = dens[:, i * TILE : (i + 1) * TILE]


def stack_kernel(*refs):
    blocks, stacks, clock, sems = refs[:8], refs[8:10], refs[10], refs[11]
    clock[...] = jnp.zeros_like(clock)

    def tick(_, carry):
        clock[...] = clock[...] + 1.0
        return carry

    lax.fori_loop(0, PAUSE, tick, 0)
    copies = [
        pltpu.make_async_copy(blocks[i], stacks[i // 4].at[i % 4], sems.at[i]) for i in range(8)
    ]
    for copy in copies:
        copy.start()
    for copy in copies:
        copy.wait()


def spread_kernel(table, panels, out, mine, sems):
    table = Table(table)
    ids, lists, orders = table.ids, table.lists, table.orders
    mine[...] = jnp.zeros_like(mine)
    for k in range(ROWS):
        s = ids[1] * ROWS + k
        for i in range(MAXT):
            group = lists[s * MAXT + i] // CT

            @pl.when((i < orders[s]) & (group // (RT // CT) == ids[0]))
            def _():
                mine[k, group % (RT // CT)] = panels[k, i]

    copies = [pltpu.make_async_copy(mine, out.at[c], sems.at[c]) for c in range(COLS)]
    for copy in copies:
        copy.start()
    for copy in copies:
        copy.wait()


def hp_kernel(table, a0, a1, a2, a3, b0, b1, b2, b3, panels, hp, pt, wide):
    table = Table(table)
    ids, lists, orders, pattern = table.ids, table.lists, table.orders, table.pattern
    half = RT * TILE // 2
    c0 = ids[1] // 4
    c1 = ids[1] % 4
    for k in range(4):
        for m in range(4):
            first = (c0 + k) % 4 * 4 + (c1 + m) % 4
            second = (c0 + m) % 4 * 4 + (c1 + k) % 4
            for part, ref, col in ((0, (a0, a1, a2, a3)[k], first), (1, (b0, b1, b2, b3)[k], second)):
                for i in range(RT // 2):
                    for j in range(CT):
                        a = part * (RT // 2) + i
                        b = col * CT + j
                        tile = ref[m, pl.ds(i * TILE, TILE), pl.ds(j * TILE, TILE)]
                        live = kept(pattern, ids[0] * RT + a, b)
                        wide[
                            pl.ds(a * TILE, TILE), pl.ds(pl.multiple_of(b * TILE, TILE), TILE)
                        ] = jnp.where(live, tile, jnp.zeros_like(tile))
    pt[...] = jnp.zeros_like(pt)
    for k in range(ROWS):
        s = ids[1] * ROWS + k
        for i in range(MAXT):

            @pl.when(i < orders[s])
            def _():
                where = pl.multiple_of(lists[s * MAXT + i] * TILE, TILE)
                pt[pl.ds(k * CW, CW), pl.ds(where, TILE)] = panels[k, i]

    hp[...] = lax.dot_general(
        wide[...], pt[...], (((1,), (1,)), ((), ())), preferred_element_type=F32
    ).astype(BF16)


def final_kernel(table, present, pieces, *refs):
    blocks = refs[:8]
    density, php, pt, hp = refs[8:]
    ids = Table(table).ids
    join_rows(ids, blocks, hp)

    def place(c, _):
        for r in range(ROWS):
            s = c * ROWS + r
            here = pl.ds(pl.multiple_of(s * CW, CW), CW)
            for g in range(RT // CT):
                piece = pieces[c, r, g]
                for a in range(g * CT, g * CT + CT):
                    live = present[s * RT + a] > 0
                    pt[here, pl.ds(a * TILE, TILE)] = jnp.where(live, piece, jnp.zeros_like(piece))
        return 0

    lax.fori_loop(0, COLS, place, 0)
    php[...] = lax.dot_general(
        pt[...], hp[...], (((0,), (0,)), ((), ())), preferred_element_type=F32
    )
    mine = pt[pl.ds(pl.multiple_of(ids[1] * WIDTH, WIDTH), WIDTH), :]
    density[...] = mine.T


def from_ring(x, axis):
    return [x] + [lax.ppermute(x, axis, [((i + k) % 4, i) for i in range(4)]) for k in range(1, 4)]


def swapped(x):
    return lax.ppermute(x, "core", [(0, 1), (1, 0)])


SMEM = pl.BlockSpec(memory_space=pltpu.SMEM)
LOCAL = pl.BlockSpec(memory_space=pltpu.VMEM)
FAR = pl.BlockSpec(memory_space=pl.ANY)


def call(kernel, outs, scratch, small, large, specs=LOCAL, space=pltpu.VMEM):
    return pl.pallas_call(
        kernel,
        out_shape=outs,
        in_specs=[SMEM] * len(small) + [LOCAL if space is pltpu.VMEM else FAR] * len(large),
        out_specs=specs,
        scratch_shapes=scratch,
        compiler_params=pltpu.CompilerParams(vmem_limit_bytes=24 << 20),
    )(*small, *[pltpu.with_memory_space_constraint(x, space) for x in large])


def call_solve(table, shift, tiles, first):
    return call(
        solve_kernel,
        pltpu.VMEM((MAXT, CW, TILE), BF16),
        [pltpu.VMEM((N, N), BF16)] * 3,
        (table, shift),
        (tiles, first),
    )


def steps(hamiltonian, pattern, tile_lists, orders, shift):
    row = lax.axis_index(ROW)
    col = lax.axis_index(COL)
    ids = jnp.stack([row, col]).astype(jnp.int32)
    table = jnp.concatenate([tile_lists.reshape(-1), orders, pattern.reshape(-1), ids])
    half = RT * TILE // 2
    top, bottom = hamiltonian[:half], hamiltonian[half:]
    strip = from_ring(hamiltonian, "z")
    ahead = from_ring(top, "c1")
    across = from_ring(bottom, "c0")
    strip = strip + [swapped(x) for x in strip]
    packed, first = call(
        pack_kernel,
        (pltpu.HBM((COLS, 4, TILE, TILE), BF16), pltpu.HBM((MAXT, TILE, TILE), BF16)),
        [pltpu.VMEM((NB * TILE, WIDTH), BF16), pltpu.SemaphoreType.DMA((COLS + 2, 4))],
        (table,),
        (top, bottom, *strip[1:]),
        (FAR, FAR),
    )
    tiles = lax.all_to_all(packed, COL, 0, 0, tiled=True)
    ahead, across = call(
        stack_kernel,
        (pltpu.HBM((4, half, WIDTH), BF16), pltpu.HBM((4, half, WIDTH), BF16)),
        [pltpu.VMEM((8, TILE), F32), pltpu.SemaphoreType.DMA((8,))],
        (),
        (*ahead, *across),
        (FAR, FAR),
        pltpu.HBM,
    )
    ahead = from_ring(ahead, "c0")
    across = from_ring(across, "c1")
    panel = call_solve(table, shift, tiles, first)
    panels = lax.all_gather(panel, ROW, axis=0, tiled=False)
    spread = call(
        spread_kernel,
        pltpu.HBM((COLS, ROWS, RT // CT, CW, TILE), BF16),
        [pltpu.VMEM((ROWS, RT // CT, CW, TILE), BF16), pltpu.SemaphoreType.DMA((COLS,))],
        (table,),
        (panels,),
        FAR,
    )
    arrived = lax.all_to_all(spread, COL, 0, 0, tiled=True)
    hp = call(
        hp_kernel,
        pltpu.VMEM((RT * TILE, WIDTH), BF16),
        [pltpu.VMEM((WIDTH, NB * TILE), BF16), pltpu.VMEM((RT * TILE, NB * TILE), BF16)],
        (table,),
        (*ahead, *across, panels),
    )
    ours = from_ring(hp, "z")
    theirs = [swapped(x) for x in ours]
    own = row * RT + jnp.arange(RT, dtype=jnp.int32)
    live = jnp.arange(MAXT, dtype=jnp.int32)[None, :] < orders[:, None]
    present = jnp.any((tile_lists[:, None, :] == own[None, :, None]) & live[:, None, :], axis=2)
    density, php = call(
        final_kernel,
        (
            jax.ShapeDtypeStruct((RT * TILE, WIDTH), BF16),
            jax.ShapeDtypeStruct((RT * TILE, WIDTH), F32),
        ),
        [pltpu.VMEM((NB * TILE, RT * TILE), BF16), pltpu.VMEM((NB * TILE, WIDTH), BF16)],
        (table, present.astype(jnp.int32).reshape(-1)),
        (arrived, *ours, *theirs),
        (LOCAL, LOCAL),
    )
    return density, php


def solution(mesh):
    fine = Mesh(mesh.devices.reshape(4, 2, 4, 4), ("z", "core", "c0", "c1"))
    split = P(ROW, COL)
    return jax.shard_map(
        steps,
        mesh=fine,
        in_specs=(split, P(), P(), P(), P()),
        out_specs=(split, split),
        check_vma=False,
    )
```

```python
import jax
import jax.numpy as jnp
from jax import lax
from jax.experimental import pallas as pl
from jax.experimental.pallas import tpu as pltpu
from jax.sharding import Mesh
from jax.sharding import PartitionSpec as P

TILE = 128
MAXT = 8
NB = 32
ROWS = 8
COLS = 16
SUBS = 128
CW = 32
PAUSE = 2200
N = MAXT * TILE
RT = NB // ROWS
CT = NB // COLS
WIDTH = CT * TILE
ROW = ("z", "core")
COL = ("c0", "c1")
F32 = jnp.float32
BF16 = jnp.bfloat16


class Table:
    def __init__(self, ref):
        self.lists = Part(ref, 0)
        self.orders = Part(ref, SUBS * MAXT)
        self.pattern = Part(ref, SUBS * MAXT + SUBS)
        self.ids = Part(ref, SUBS * MAXT + SUBS + NB * NB)


class Part:
    def __init__(self, ref, base):
        self.ref = ref
        self.base = base

    def __getitem__(self, index):
        return self.ref[self.base + index]


def kept(pattern, a, b):
    return (pattern[a * NB + b] > 0) | (a == b)


def ring_owner(ids, k, part):
    return (ids[0] // 2 + k) % 4 * 2 + (ids[0] + part) % 2


def join_rows(ids, blocks, whole):
    for part in range(2):
        for k in range(4):
            block = blocks[part * 4 + k]
            pieces = block if isinstance(block, tuple) else (block,)
            size = RT * TILE // len(pieces)
            start = ring_owner(ids, k, part) * RT * TILE
            for number, piece in enumerate(pieces):
                whole[pl.ds(pl.multiple_of(start + number * size, size), size), :] = piece[...]


def cyclic(j, k):
    return 1 + (j - 1 + k) % (MAXT - 1)


def pack_kernel(table, *refs):
    table = Table(table)
    ids, lists, orders = table.ids, table.lists, table.orders
    halves, blocks, (out, first, strip, sems) = refs[:2], refs[2:9], refs[9:]
    join_rows(ids, (halves, *blocks), strip)

    def send(c, k, row, lanes):
        start = pl.multiple_of(row * TILE, TILE)
        lanes = pl.ds(pl.multiple_of(lanes * TILE, TILE), TILE)
        return pltpu.make_async_copy(
            strip.at[pl.ds(start, TILE), lanes], out.at[c, k], sems.at[c, k]
        )

    def one(c, _):
        s = c * ROWS + ids[0]
        which = jnp.int32(1)
        for j in range(2, MAXT):
            hit = (lists[s * MAXT + j] // CT == ids[1]) & (j < orders[s])
            which = jnp.where(hit, j, which)
        side = lists[s * MAXT + which] % CT
        for k in range(4):
            send(c, k, lists[s * MAXT + cyclic(which, k)], side).start()
        return 0

    lax.fori_loop(0, COLS, one, 0)

    own = (ids[1] * ROWS + ids[0]) * MAXT
    side = pl.ds(pl.multiple_of(lists[own] % CT * TILE, TILE), TILE)
    heads = [
        pltpu.make_async_copy(
            strip.at[pl.ds(pl.multiple_of(lists[own + i] * TILE, TILE), TILE), side],
            first.at[i],
            sems.at[COLS + i // 4, i % 4],
        )
        for i in range(MAXT)
    ]
    for copy in heads:
        copy.start()

    def done(c, _):
        for k in range(4):
            send(c, k, 0, 0).wait()
        return 0

    lax.fori_loop(0, COLS, done, 0)
    for copy in heads:
        copy.wait()


def solve_kernel(table, shift, tiles, first, panel, x, f, y):
    table = Table(table)
    ids, lists, pattern = table.ids, table.lists, table.pattern
    s = ids[1] * ROWS + ids[0]
    order = table.orders[s]
    potential = shift[0]
    names = [lists[s * MAXT + j] for j in range(MAXT)]
    rows = lax.broadcasted_iota(jnp.int32, (TILE, TILE), 0)
    cols = lax.broadcasted_iota(jnp.int32, (TILE, TILE), 1)
    eye = jnp.where(rows == cols, 1.0, 0.0).astype(F32)

    def put(i, j, tile):
        y[pl.ds(i * TILE, TILE), pl.ds(j * TILE, TILE)] = tile

    def masked(i, j, tile):
        both = kept(pattern, names[i], names[j]) & (i < order) & (j < order)
        return jnp.where(both, tile, jnp.zeros_like(tile))

    for i in range(MAXT):
        tile = masked(i, 0, first[i])
        put(i, 0, tile)
        if i:
            put(0, i, tile.T)
            for k in range(4):
                tile = masked(cyclic(i, k), i, tiles[names[i] // CT, k])
                put(cyclic(i, k), i, tile)
                if k:
                    put(i, cyclic(i, k), tile.T)

    def shifted(i, j):
        tile = y[pl.ds(i * TILE, TILE), pl.ds(j * TILE, TILE)].astype(F32)
        if i == j:
            tile = tile - jnp.where(i < order, potential, 0.0) * eye
        return tile

    largest = jnp.zeros((), F32)
    for i in range(MAXT):
        total = jnp.zeros((TILE, TILE), F32)
        for j in range(MAXT):
            tile = shifted(i, j)
            total = total + tile * tile
        largest = jnp.maximum(largest, jnp.max(jnp.sum(total, axis=1)))
    root = jnp.sqrt(jnp.full((8, TILE), largest + 1e-06, F32))
    inverse = (1.0 / (jnp.abs(potential) + 2.0 * root))[0:1, :]
    for i in range(MAXT):
        for j in range(MAXT):
            x[pl.ds(i * TILE, TILE), pl.ds(j * TILE, TILE)] = (shifted(i, j) * inverse).astype(BF16)

    band = 256
    brow = lax.broadcasted_iota(jnp.int32, (band, N), 0)
    bcol = lax.broadcasted_iota(jnp.int32, (band, N), 1)

    def step(source, target):
        blocks = N // band
        for b in range(blocks):
            here = slice(b * band, b * band + band)
            rest = slice(b * band, N)
            q = lax.dot_general(
                source[here, :], source[:, rest], (((1,), (0,)), ((), ())), preferred_element_type=F32
            )
            diag = jnp.where(brow[:, : N - b * band] == bcol[:, : N - b * band], 1.5, 0.0)
            part = (diag - 0.5 * q).astype(BF16)
            f[here, rest] = part
            for c in range(b + 1, blocks):
                f[c * band : c * band + band, here] = part[:, (c - b) * band : (c - b + 1) * band].T
        for b in range(blocks):
            here = slice(b * band, b * band + band)
            rest = slice(b * band, N)
            part = jnp.dot(source[here, :], f[:, rest], preferred_element_type=F32).astype(BF16)
            target[here, rest] = part
            for c in range(b + 1, blocks):
                target[c * band : c * band + band, here] = part[
                    :, (c - b) * band : (c - b + 1) * band
                ].T

    step(x, y)
    step(y, x)
    offset = pl.multiple_of(s % (TILE // CW) * CW, CW)
    prow = lax.broadcasted_iota(jnp.int32, (CW, N), 0) + offset
    pcol = lax.broadcasted_iota(jnp.int32, (CW, N), 1)
    q = jnp.dot(x[pl.ds(offset, CW), :], x[...], preferred_element_type=F32)
    part = (jnp.where(prow == pcol, 1.5, 0.0) - 0.5 * q).astype(BF16)
    z = jnp.dot(part, x[...], preferred_element_type=F32)
    dens = (jnp.where(prow == pcol, 0.5, 0.0) - 0.5 * z).astype(BF16)
    for i in range(MAXT):
        panel[i] = dens[:, i * TILE : (i + 1) * TILE]


def pause_kernel(shift, out):
    out[...] = jnp.full_like(out, jnp.abs(shift[0]))

    def tick(_, carry):
        out[...] = out[...] + 1.0
        return carry

    lax.fori_loop(0, PAUSE, tick, 0)


def spread_kernel(table, panels, out, mine, sems):
    table = Table(table)
    ids, lists, orders = table.ids, table.lists, table.orders
    mine[...] = jnp.zeros_like(mine)
    for k in range(ROWS):
        s = ids[1] * ROWS + k
        for i in range(MAXT):
            group = lists[s * MAXT + i] // CT

            @pl.when((i < orders[s]) & (group // (RT // CT) == ids[0]))
            def _():
                mine[k, group % (RT // CT)] = panels[k, i]

    copies = [pltpu.make_async_copy(mine, out.at[c], sems.at[c]) for c in range(COLS)]
    for copy in copies:
        copy.start()
    for copy in copies:
        copy.wait()


def hp_kernel(table, a0, a1, a2, a3, b0, b1, b2, b3, panels, hp, pt, wide):
    table = Table(table)
    ids, lists, orders, pattern = table.ids, table.lists, table.orders, table.pattern
    half = RT * TILE // 2
    c0 = ids[1] // 4
    c1 = ids[1] % 4
    for k in range(4):
        for m in range(4):
            first = (c0 + k) % 4 * 4 + (c1 + m) % 4
            second = (c0 + m) % 4 * 4 + (c1 + k) % 4
            for part, ref, col in ((0, (a0, a1, a2, a3)[k], first), (1, (b0, b1, b2, b3)[k], second)):
                for i in range(RT // 2):
                    for j in range(CT):
                        a = part * (RT // 2) + i
                        b = col * CT + j
                        tile = ref[m, pl.ds(i * TILE, TILE), pl.ds(j * TILE, TILE)]
                        live = kept(pattern, ids[0] * RT + a, b)
                        wide[
                            pl.ds(a * TILE, TILE), pl.ds(pl.multiple_of(b * TILE, TILE), TILE)
                        ] = jnp.where(live, tile, jnp.zeros_like(tile))
    pt[...] = jnp.zeros_like(pt)
    for k in range(ROWS):
        s = ids[1] * ROWS + k
        for i in range(MAXT):

            @pl.when(i < orders[s])
            def _():
                where = pl.multiple_of(lists[s * MAXT + i] * TILE, TILE)
                pt[pl.ds(k * CW, CW), pl.ds(where, TILE)] = panels[k, i]

    hp[...] = lax.dot_general(
        wide[...], pt[...], (((1,), (1,)), ((), ())), preferred_element_type=F32
    ).astype(BF16)


def final_kernel(table, present, pieces, *refs):
    blocks = refs[:8]
    density, php, pt, hp = refs[8:]
    ids = Table(table).ids
    join_rows(ids, blocks, hp)

    def place(c, _):
        for r in range(ROWS):
            s = c * ROWS + r
            here = pl.ds(pl.multiple_of(s * CW, CW), CW)
            for g in range(RT // CT):
                piece = pieces[c, r, g]
                for a in range(g * CT, g * CT + CT):
                    live = present[s * RT + a] > 0
                    pt[here, pl.ds(a * TILE, TILE)] = jnp.where(live, piece, jnp.zeros_like(piece))
        return 0

    lax.fori_loop(0, COLS, place, 0)
    php[...] = lax.dot_general(
        pt[...], hp[...], (((0,), (0,)), ((), ())), preferred_element_type=F32
    )
    mine = pt[pl.ds(pl.multiple_of(ids[1] * WIDTH, WIDTH), WIDTH), :]
    density[...] = mine.T


def from_ring(x, axis):
    return [x] + [lax.ppermute(x, axis, [((i + k) % 4, i) for i in range(4)]) for k in range(1, 4)]


def swapped(x):
    return lax.ppermute(x, "core", [(0, 1), (1, 0)])


SMEM = pl.BlockSpec(memory_space=pltpu.SMEM)
LOCAL = pl.BlockSpec(memory_space=pltpu.VMEM)
FAR = pl.BlockSpec(memory_space=pl.ANY)


def call(kernel, outs, scratch, small, large, specs=LOCAL, space=pltpu.VMEM):
    return pl.pallas_call(
        kernel,
        out_shape=outs,
        in_specs=[SMEM] * len(small) + [LOCAL if space is pltpu.VMEM else FAR] * len(large),
        out_specs=specs,
        scratch_shapes=scratch,
        compiler_params=pltpu.CompilerParams(vmem_limit_bytes=24 << 20),
    )(*small, *[pltpu.with_memory_space_constraint(x, space) for x in large])


def call_solve(table, shift, tiles, first):
    return call(
        solve_kernel,
        pltpu.VMEM((MAXT, CW, TILE), BF16),
        [pltpu.VMEM((N, N), BF16)] * 3,
        (table, shift),
        (tiles, first),
    )


def steps(hamiltonian, pattern, tile_lists, orders, shift):
    row = lax.axis_index(ROW)
    col = lax.axis_index(COL)
    ids = jnp.stack([row, col]).astype(jnp.int32)
    table = jnp.concatenate([tile_lists.reshape(-1), orders, pattern.reshape(-1), ids])
    half = RT * TILE // 2
    top, bottom = hamiltonian[:half], hamiltonian[half:]
    strip = from_ring(hamiltonian, "z")
    ahead = from_ring(top, "c1")
    across = from_ring(bottom, "c0")
    strip = strip + [swapped(x) for x in strip]
    packed, first = call(
        pack_kernel,
        (pltpu.HBM((COLS, 4, TILE, TILE), BF16), pltpu.HBM((MAXT, TILE, TILE), BF16)),
        [pltpu.VMEM((NB * TILE, WIDTH), BF16), pltpu.SemaphoreType.DMA((COLS + 2, 4))],
        (table,),
        (top, bottom, *strip[1:]),
        (FAR, FAR),
    )
    packed, late = lax.optimization_barrier((packed, shift))
    tiles = lax.all_to_all(packed, COL, 0, 0, tiled=True)
    clock = call(pause_kernel, pltpu.VMEM((8, TILE), F32), [], (late,), ())
    go = clock[0, 0] >= 0.0
    ahead = jnp.stack(ahead[:1] + [jnp.where(go, x, jnp.zeros_like(x)) for x in ahead[1:]])
    across = jnp.stack(across[:1] + [jnp.where(go, x, jnp.zeros_like(x)) for x in across[1:]])
    ahead = from_ring(ahead, "c0")
    across = from_ring(across, "c1")
    panel = call_solve(table, shift, tiles, first)
    panels = lax.all_gather(panel, ROW, axis=0, tiled=False)
    spread = call(
        spread_kernel,
        pltpu.HBM((COLS, ROWS, RT // CT, CW, TILE), BF16),
        [pltpu.VMEM((ROWS, RT // CT, CW, TILE), BF16), pltpu.SemaphoreType.DMA((COLS,))],
        (table,),
        (panels,),
        FAR,
    )
    arrived = lax.all_to_all(spread, COL, 0, 0, tiled=True)
    hp = call(
        hp_kernel,
        pltpu.VMEM((RT * TILE, WIDTH), BF16),
        [pltpu.VMEM((WIDTH, NB * TILE), BF16), pltpu.VMEM((RT * TILE, NB * TILE), BF16)],
        (table,),
        (*ahead, *across, panels),
    )
    ours = from_ring(hp, "z")
    theirs = [swapped(x) for x in ours]
    own = row * RT + jnp.arange(RT, dtype=jnp.int32)
    live = jnp.arange(MAXT, dtype=jnp.int32)[None, :] < orders[:, None]
    present = jnp.any((tile_lists[:, None, :] == own[None, :, None]) & live[:, None, :], axis=2)
    density, php = call(
        final_kernel,
        (
            jax.ShapeDtypeStruct((RT * TILE, WIDTH), BF16),
            jax.ShapeDtypeStruct((RT * TILE, WIDTH), F32),
        ),
        [pltpu.VMEM((NB * TILE, RT * TILE), BF16), pltpu.VMEM((NB * TILE, WIDTH), BF16)],
        (table, present.astype(jnp.int32).reshape(-1)),
        (arrived, *ours, *theirs),
        (LOCAL, LOCAL),
    )
    return density, php


def solution(mesh):
    fine = Mesh(mesh.devices.reshape(4, 2, 4, 4), ("z", "core", "c0", "c1"))
    split = P(ROW, COL)
    return jax.shard_map(
        steps,
        mesh=fine,
        in_specs=(split, P(), P(), P(), P()),
        out_specs=(split, split),
        check_vma=False,
    )
```

```python
import jax
import jax.numpy as jnp
from jax import lax
from jax.experimental import pallas as pl
from jax.experimental.pallas import tpu as pltpu
from jax.sharding import Mesh
from jax.sharding import PartitionSpec as P

TILE = 128
MAXT = 8
NB = 32
ROWS = 8
COLS = 16
SUBS = 128
CW = 32
N = MAXT * TILE
RT = NB // ROWS
CT = NB // COLS
WIDTH = CT * TILE
ROW = ("z", "core")
COL = ("c0", "c1")
F32 = jnp.float32
BF16 = jnp.bfloat16


class Table:
    def __init__(self, ref):
        self.lists = Part(ref, 0)
        self.orders = Part(ref, SUBS * MAXT)
        self.pattern = Part(ref, SUBS * MAXT + SUBS)
        self.ids = Part(ref, SUBS * MAXT + SUBS + NB * NB)


class Part:
    def __init__(self, ref, base):
        self.ref = ref
        self.base = base

    def __getitem__(self, index):
        return self.ref[self.base + index]


def kept(pattern, a, b):
    return (pattern[a * NB + b] > 0) | (a == b)


def ring_owner(ids, k, part):
    return (ids[0] // 2 + k) % 4 * 2 + (ids[0] + part) % 2


def join_rows(ids, blocks, whole):
    for part in range(2):
        for k in range(4):
            block = blocks[part * 4 + k]
            pieces = block if isinstance(block, tuple) else (block,)
            size = RT * TILE // len(pieces)
            start = ring_owner(ids, k, part) * RT * TILE
            for number, piece in enumerate(pieces):
                whole[pl.ds(pl.multiple_of(start + number * size, size), size), :] = piece[...]


def cyclic(j, k):
    return 1 + (j - 1 + k) % (MAXT - 1)


def pack_kernel(table, *refs):
    table = Table(table)
    ids, lists, orders = table.ids, table.lists, table.orders
    halves, blocks, (out, first, strip, sems) = refs[:2], refs[2:9], refs[9:]
    join_rows(ids, (halves, *blocks), strip)

    def send(c, k, row, lanes):
        start = pl.multiple_of(row * TILE, TILE)
        lanes = pl.ds(pl.multiple_of(lanes * TILE, TILE), TILE)
        return pltpu.make_async_copy(
            strip.at[pl.ds(start, TILE), lanes], out.at[c, k], sems.at[c, k]
        )

    def one(c, _):
        s = c * ROWS + ids[0]
        which = jnp.int32(1)
        for j in range(2, MAXT):
            hit = (lists[s * MAXT + j] // CT == ids[1]) & (j < orders[s])
            which = jnp.where(hit, j, which)
        side = lists[s * MAXT + which] % CT
        for k in range(4):
            send(c, k, lists[s * MAXT + cyclic(which, k)], side).start()
        return 0

    lax.fori_loop(0, COLS, one, 0)

    own = (ids[1] * ROWS + ids[0]) * MAXT
    side = pl.ds(pl.multiple_of(lists[own] % CT * TILE, TILE), TILE)
    heads = [
        pltpu.make_async_copy(
            strip.at[pl.ds(pl.multiple_of(lists[own + i] * TILE, TILE), TILE), side],
            first.at[i],
            sems.at[COLS + i // 4, i % 4],
        )
        for i in range(MAXT)
    ]
    for copy in heads:
        copy.start()

    def done(c, _):
        for k in range(4):
            send(c, k, 0, 0).wait()
        return 0

    lax.fori_loop(0, COLS, done, 0)
    for copy in heads:
        copy.wait()


def solve_kernel(table, shift, tiles, first, panel, x, f, y):
    table = Table(table)
    ids, lists, pattern = table.ids, table.lists, table.pattern
    s = ids[1] * ROWS + ids[0]
    order = table.orders[s]
    potential = shift[0]
    names = [lists[s * MAXT + j] for j in range(MAXT)]
    rows = lax.broadcasted_iota(jnp.int32, (TILE, TILE), 0)
    cols = lax.broadcasted_iota(jnp.int32, (TILE, TILE), 1)
    eye = jnp.where(rows == cols, 1.0, 0.0).astype(F32)

    def put(i, j, tile):
        y[pl.ds(i * TILE, TILE), pl.ds(j * TILE, TILE)] = tile

    def masked(i, j, tile):
        both = kept(pattern, names[i], names[j]) & (i < order) & (j < order)
        return jnp.where(both, tile, jnp.zeros_like(tile))

    for i in range(MAXT):
        tile = masked(i, 0, first[i])
        put(i, 0, tile)
        if i:
            put(0, i, tile.T)
            for k in range(4):
                tile = masked(cyclic(i, k), i, tiles[names[i] // CT, k])
                put(cyclic(i, k), i, tile)
                if k:
                    put(i, cyclic(i, k), tile.T)

    def shifted(i, j):
        tile = y[pl.ds(i * TILE, TILE), pl.ds(j * TILE, TILE)].astype(F32)
        if i == j:
            tile = tile - jnp.where(i < order, potential, 0.0) * eye
        return tile

    largest = jnp.zeros((), F32)
    for i in range(MAXT):
        total = jnp.zeros((TILE, TILE), F32)
        for j in range(MAXT):
            tile = shifted(i, j)
            total = total + tile * tile
        largest = jnp.maximum(largest, jnp.max(jnp.sum(total, axis=1)))
    root = jnp.sqrt(jnp.full((8, TILE), largest + 1e-06, F32))
    inverse = (1.0 / (jnp.abs(potential) + 2.0 * root))[0:1, :]
    for i in range(MAXT):
        for j in range(MAXT):
            x[pl.ds(i * TILE, TILE), pl.ds(j * TILE, TILE)] = (shifted(i, j) * inverse).astype(BF16)

    band = 256
    brow = lax.broadcasted_iota(jnp.int32, (band, N), 0)
    bcol = lax.broadcasted_iota(jnp.int32, (band, N), 1)

    def step(source, target):
        blocks = N // band
        for b in range(blocks):
            here = slice(b * band, b * band + band)
            rest = slice(b * band, N)
            q = lax.dot_general(
                source[here, :], source[:, rest], (((1,), (0,)), ((), ())), preferred_element_type=F32
            )
            diag = jnp.where(brow[:, : N - b * band] == bcol[:, : N - b * band], 1.5, 0.0)
            part = (diag - 0.5 * q).astype(BF16)
            f[here, rest] = part
            for c in range(b + 1, blocks):
                f[c * band : c * band + band, here] = part[:, (c - b) * band : (c - b + 1) * band].T
        for b in range(blocks):
            here = slice(b * band, b * band + band)
            rest = slice(b * band, N)
            part = jnp.dot(source[here, :], f[:, rest], preferred_element_type=F32).astype(BF16)
            target[here, rest] = part
            for c in range(b + 1, blocks):
                target[c * band : c * band + band, here] = part[
                    :, (c - b) * band : (c - b + 1) * band
                ].T

    step(x, y)
    step(y, x)
    offset = pl.multiple_of(s % (TILE // CW) * CW, CW)
    prow = lax.broadcasted_iota(jnp.int32, (CW, N), 0) + offset
    pcol = lax.broadcasted_iota(jnp.int32, (CW, N), 1)
    q = jnp.dot(x[pl.ds(offset, CW), :], x[...], preferred_element_type=F32)
    part = (jnp.where(prow == pcol, 1.5, 0.0) - 0.5 * q).astype(BF16)
    z = jnp.dot(part, x[...], preferred_element_type=F32)
    dens = (jnp.where(prow == pcol, 0.5, 0.0) - 0.5 * z).astype(BF16)
    for i in range(MAXT):
        panel[i] = dens[:, i * TILE : (i + 1) * TILE]


def spread_kernel(table, panels, out, mine, sems):
    table = Table(table)
    ids, lists, orders = table.ids, table.lists, table.orders
    mine[...] = jnp.zeros_like(mine)
    for k in range(ROWS):
        s = ids[1] * ROWS + k
        for i in range(MAXT):
            group = lists[s * MAXT + i] // CT

            @pl.when((i < orders[s]) & (group // (RT // CT) == ids[0]))
            def _():
                mine[k, group % (RT // CT)] = panels[k, i]

    copies = [pltpu.make_async_copy(mine, out.at[c], sems.at[c]) for c in range(COLS)]
    for copy in copies:
        copy.start()
    for copy in copies:
        copy.wait()


def hp_kernel(table, a0, a1, a2, a3, b0, b1, b2, b3, panels, hp, pt, wide):
    table = Table(table)
    ids, lists, orders, pattern = table.ids, table.lists, table.orders, table.pattern
    half = RT * TILE // 2
    c0 = ids[1] // 4
    c1 = ids[1] % 4
    for k in range(4):
        for m in range(4):
            first = (c0 + k) % 4 * 4 + (c1 + m) % 4
            second = (c0 + m) % 4 * 4 + (c1 + k) % 4
            for part, ref, col in ((0, (a0, a1, a2, a3)[k], first), (1, (b0, b1, b2, b3)[k], second)):
                for i in range(RT // 2):
                    for j in range(CT):
                        a = part * (RT // 2) + i
                        b = col * CT + j
                        tile = ref[m, pl.ds(i * TILE, TILE), pl.ds(j * TILE, TILE)]
                        live = kept(pattern, ids[0] * RT + a, b)
                        wide[
                            pl.ds(a * TILE, TILE), pl.ds(pl.multiple_of(b * TILE, TILE), TILE)
                        ] = jnp.where(live, tile, jnp.zeros_like(tile))
    pt[...] = jnp.zeros_like(pt)
    for k in range(ROWS):
        s = ids[1] * ROWS + k
        for i in range(MAXT):

            @pl.when(i < orders[s])
            def _():
                where = pl.multiple_of(lists[s * MAXT + i] * TILE, TILE)
                pt[pl.ds(k * CW, CW), pl.ds(where, TILE)] = panels[k, i]

    hp[...] = lax.dot_general(
        wide[...], pt[...], (((1,), (1,)), ((), ())), preferred_element_type=F32
    ).astype(BF16)


def final_kernel(table, present, pieces, *refs):
    blocks = refs[:8]
    density, php, pt, hp = refs[8:]
    ids = Table(table).ids
    join_rows(ids, blocks, hp)

    def place(c, _):
        for r in range(ROWS):
            s = c * ROWS + r
            here = pl.ds(pl.multiple_of(s * CW, CW), CW)
            for g in range(RT // CT):
                piece = pieces[c, r, g]
                for a in range(g * CT, g * CT + CT):
                    live = present[s * RT + a] > 0
                    pt[here, pl.ds(a * TILE, TILE)] = jnp.where(live, piece, jnp.zeros_like(piece))
        return 0

    lax.fori_loop(0, COLS, place, 0)
    php[...] = lax.dot_general(
        pt[...], hp[...], (((0,), (0,)), ((), ())), preferred_element_type=F32
    )
    mine = pt[pl.ds(pl.multiple_of(ids[1] * WIDTH, WIDTH), WIDTH), :]
    density[...] = mine.T


def from_ring(x, axis):
    return [x] + [lax.ppermute(x, axis, [((i + k) % 4, i) for i in range(4)]) for k in range(1, 4)]


def swapped(x):
    return lax.ppermute(x, "core", [(0, 1), (1, 0)])


SMEM = pl.BlockSpec(memory_space=pltpu.SMEM)
LOCAL = pl.BlockSpec(memory_space=pltpu.VMEM)
FAR = pl.BlockSpec(memory_space=pl.ANY)


def call(kernel, outs, scratch, small, large, specs=LOCAL, space=pltpu.VMEM):
    return pl.pallas_call(
        kernel,
        out_shape=outs,
        in_specs=[SMEM] * len(small) + [LOCAL if space is pltpu.VMEM else FAR] * len(large),
        out_specs=specs,
        scratch_shapes=scratch,
        compiler_params=pltpu.CompilerParams(vmem_limit_bytes=24 << 20),
    )(*small, *[pltpu.with_memory_space_constraint(x, space) for x in large])


def call_solve(table, shift, tiles, first):
    return call(
        solve_kernel,
        pltpu.VMEM((MAXT, CW, TILE), BF16),
        [pltpu.VMEM((N, N), BF16)] * 3,
        (table, shift),
        (tiles, first),
    )


def steps(hamiltonian, pattern, tile_lists, orders, shift):
    row = lax.axis_index(ROW)
    col = lax.axis_index(COL)
    ids = jnp.stack([row, col]).astype(jnp.int32)
    table = jnp.concatenate([tile_lists.reshape(-1), orders, pattern.reshape(-1), ids])
    half = RT * TILE // 2
    top, bottom = hamiltonian[:half], hamiltonian[half:]
    strip = from_ring(hamiltonian, "z")
    across = from_ring(bottom, "c0")
    ahead = from_ring(top, "c1")
    strip = strip + [swapped(x) for x in strip]
    packed, first = call(
        pack_kernel,
        (pltpu.HBM((COLS, 4, TILE, TILE), BF16), pltpu.HBM((MAXT, TILE, TILE), BF16)),
        [pltpu.VMEM((NB * TILE, WIDTH), BF16), pltpu.SemaphoreType.DMA((COLS + 2, 4))],
        (table,),
        (top, bottom, *strip[1:]),
        (FAR, FAR),
    )
    packed, ahead, across = lax.optimization_barrier((packed, ahead, across))
    tiles = lax.all_to_all(packed, COL, 0, 0, tiled=True)
    across = from_ring(jnp.stack(across), "c1")
    ahead = from_ring(jnp.stack(ahead), "c0")
    panel = call_solve(table, shift, tiles, first)
    panels = lax.all_gather(panel, ROW, axis=0, tiled=False)
    spread = call(
        spread_kernel,
        pltpu.HBM((COLS, ROWS, RT // CT, CW, TILE), BF16),
        [pltpu.VMEM((ROWS, RT // CT, CW, TILE), BF16), pltpu.SemaphoreType.DMA((COLS,))],
        (table,),
        (panels,),
        FAR,
    )
    arrived = lax.all_to_all(spread, COL, 0, 0, tiled=True)
    hp = call(
        hp_kernel,
        pltpu.VMEM((RT * TILE, WIDTH), BF16),
        [pltpu.VMEM((WIDTH, NB * TILE), BF16), pltpu.VMEM((RT * TILE, NB * TILE), BF16)],
        (table,),
        (*ahead, *across, panels),
    )
    ours = from_ring(hp, "z")
    theirs = [swapped(x) for x in ours]
    own = row * RT + jnp.arange(RT, dtype=jnp.int32)
    live = jnp.arange(MAXT, dtype=jnp.int32)[None, :] < orders[:, None]
    present = jnp.any((tile_lists[:, None, :] == own[None, :, None]) & live[:, None, :], axis=2)
    density, php = call(
        final_kernel,
        (
            jax.ShapeDtypeStruct((RT * TILE, WIDTH), BF16),
            jax.ShapeDtypeStruct((RT * TILE, WIDTH), F32),
        ),
        [pltpu.VMEM((NB * TILE, RT * TILE), BF16), pltpu.VMEM((NB * TILE, WIDTH), BF16)],
        (table, present.astype(jnp.int32).reshape(-1)),
        (arrived, *ours, *theirs),
        (LOCAL, LOCAL),
    )
    return density, php


def solution(mesh):
    fine = Mesh(mesh.devices.reshape(4, 2, 4, 4), ("z", "core", "c0", "c1"))
    split = P(ROW, COL)
    return jax.shard_map(
        steps,
        mesh=fine,
        in_specs=(split, P(), P(), P(), P()),
        out_specs=(split, split),
        check_vma=False,
    )
```

```python
import jax
import jax.numpy as jnp
from jax import lax
from jax.experimental import pallas as pl
from jax.experimental.pallas import tpu as pltpu
from jax.sharding import Mesh
from jax.sharding import PartitionSpec as P

TILE = 128
MAXT = 8
NB = 32
ROWS = 8
COLS = 16
SUBS = 128
CW = 32
N = MAXT * TILE
RT = NB // ROWS
CT = NB // COLS
WIDTH = CT * TILE
ROW = ("z", "core")
COL = ("c0", "c1")
F32 = jnp.float32
BF16 = jnp.bfloat16


class Table:
    def __init__(self, ref):
        self.lists = Part(ref, 0)
        self.orders = Part(ref, SUBS * MAXT)
        self.pattern = Part(ref, SUBS * MAXT + SUBS)
        self.ids = Part(ref, SUBS * MAXT + SUBS + NB * NB)


class Part:
    def __init__(self, ref, base):
        self.ref = ref
        self.base = base

    def __getitem__(self, index):
        return self.ref[self.base + index]


def kept(pattern, a, b):
    return (pattern[a * NB + b] > 0) | (a == b)


def ring_owner(ids, k, part):
    return (ids[0] // 2 + k) % 4 * 2 + (ids[0] + part) % 2


def join_rows(ids, blocks, whole):
    for part in range(2):
        for k in range(4):
            block = blocks[part * 4 + k]
            pieces = block if isinstance(block, tuple) else (block,)
            size = RT * TILE // len(pieces)
            start = ring_owner(ids, k, part) * RT * TILE
            for number, piece in enumerate(pieces):
                whole[pl.ds(pl.multiple_of(start + number * size, size), size), :] = piece[...]


def cyclic(j, k):
    return 1 + (j - 1 + k) % (MAXT - 1)


def pack_kernel(table, *refs):
    table = Table(table)
    ids, lists, orders = table.ids, table.lists, table.orders
    halves, blocks, (out, first, strip, sems) = refs[:2], refs[2:9], refs[9:]
    join_rows(ids, (halves, *blocks), strip)

    def send(c, k, row, lanes):
        start = pl.multiple_of(row * TILE, TILE)
        lanes = pl.ds(pl.multiple_of(lanes * TILE, TILE), TILE)
        return pltpu.make_async_copy(
            strip.at[pl.ds(start, TILE), lanes], out.at[c, k], sems.at[c, k]
        )

    def one(c, _):
        s = c * ROWS + ids[0]
        which = jnp.int32(1)
        for j in range(2, MAXT):
            hit = (lists[s * MAXT + j] // CT == ids[1]) & (j < orders[s])
            which = jnp.where(hit, j, which)
        side = lists[s * MAXT + which] % CT
        for k in range(4):
            send(c, k, lists[s * MAXT + cyclic(which, k)], side).start()
        return 0

    lax.fori_loop(0, COLS, one, 0)

    own = (ids[1] * ROWS + ids[0]) * MAXT
    side = pl.ds(pl.multiple_of(lists[own] % CT * TILE, TILE), TILE)
    heads = [
        pltpu.make_async_copy(
            strip.at[pl.ds(pl.multiple_of(lists[own + i] * TILE, TILE), TILE), side],
            first.at[i],
            sems.at[COLS + i // 4, i % 4],
        )
        for i in range(MAXT)
    ]
    for copy in heads:
        copy.start()

    def done(c, _):
        for k in range(4):
            send(c, k, 0, 0).wait()
        return 0

    lax.fori_loop(0, COLS, done, 0)
    for copy in heads:
        copy.wait()


def solve_kernel(table, shift, tiles, first, panel, x, f, y):
    table = Table(table)
    ids, lists, pattern = table.ids, table.lists, table.pattern
    s = ids[1] * ROWS + ids[0]
    order = table.orders[s]
    potential = shift[0]
    names = [lists[s * MAXT + j] for j in range(MAXT)]
    rows = lax.broadcasted_iota(jnp.int32, (TILE, TILE), 0)
    cols = lax.broadcasted_iota(jnp.int32, (TILE, TILE), 1)
    eye = jnp.where(rows == cols, 1.0, 0.0).astype(F32)

    def put(i, j, tile):
        y[pl.ds(i * TILE, TILE), pl.ds(j * TILE, TILE)] = tile

    def masked(i, j, tile):
        both = kept(pattern, names[i], names[j]) & (i < order) & (j < order)
        return jnp.where(both, tile, jnp.zeros_like(tile))

    for i in range(MAXT):
        tile = masked(i, 0, first[i])
        put(i, 0, tile)
        if i:
            put(0, i, tile.T)
            for k in range(4):
                tile = masked(cyclic(i, k), i, tiles[names[i] // CT, k])
                put(cyclic(i, k), i, tile)
                if k:
                    put(i, cyclic(i, k), tile.T)

    def shifted(i, j):
        tile = y[pl.ds(i * TILE, TILE), pl.ds(j * TILE, TILE)].astype(F32)
        if i == j:
            tile = tile - jnp.where(i < order, potential, 0.0) * eye
        return tile

    largest = jnp.zeros((), F32)
    for i in range(MAXT):
        total = jnp.zeros((TILE, TILE), F32)
        for j in range(MAXT):
            tile = shifted(i, j)
            total = total + tile * tile
        largest = jnp.maximum(largest, jnp.max(jnp.sum(total, axis=1)))
    root = jnp.sqrt(jnp.full((8, TILE), largest + 1e-06, F32))
    inverse = (1.0 / (jnp.abs(potential) + 2.0 * root))[0:1, :]
    for i in range(MAXT):
        for j in range(MAXT):
            x[pl.ds(i * TILE, TILE), pl.ds(j * TILE, TILE)] = (shifted(i, j) * inverse).astype(BF16)

    band = 256
    brow = lax.broadcasted_iota(jnp.int32, (band, N), 0)
    bcol = lax.broadcasted_iota(jnp.int32, (band, N), 1)

    def step(source, target):
        blocks = N // band
        for b in range(blocks):
            here = slice(b * band, b * band + band)
            rest = slice(b * band, N)
            q = lax.dot_general(
                source[here, :], source[:, rest], (((1,), (0,)), ((), ())), preferred_element_type=F32
            )
            diag = jnp.where(brow[:, : N - b * band] == bcol[:, : N - b * band], 1.5, 0.0)
            part = (diag - 0.5 * q).astype(BF16)
            f[here, rest] = part
            for c in range(b + 1, blocks):
                f[c * band : c * band + band, here] = part[:, (c - b) * band : (c - b + 1) * band].T
        for b in range(blocks):
            here = slice(b * band, b * band + band)
            rest = slice(b * band, N)
            part = jnp.dot(source[here, :], f[:, rest], preferred_element_type=F32).astype(BF16)
            target[here, rest] = part
            for c in range(b + 1, blocks):
                target[c * band : c * band + band, here] = part[
                    :, (c - b) * band : (c - b + 1) * band
                ].T

    step(x, y)
    step(y, x)
    offset = pl.multiple_of(s % (TILE // CW) * CW, CW)
    prow = lax.broadcasted_iota(jnp.int32, (CW, N), 0) + offset
    pcol = lax.broadcasted_iota(jnp.int32, (CW, N), 1)
    q = jnp.dot(x[pl.ds(offset, CW), :], x[...], preferred_element_type=F32)
    part = (jnp.where(prow == pcol, 1.5, 0.0) - 0.5 * q).astype(BF16)
    z = jnp.dot(part, x[...], preferred_element_type=F32)
    dens = (jnp.where(prow == pcol, 0.5, 0.0) - 0.5 * z).astype(BF16)
    for i in range(MAXT):
        panel[i] = dens[:, i * TILE : (i + 1) * TILE]


def spread_kernel(table, panels, out, mine, sems):
    table = Table(table)
    ids, lists, orders = table.ids, table.lists, table.orders
    for k in range(ROWS):
        s = ids[1] * ROWS + k
        order = orders[s]
        where = [jnp.int32(-1)] * (RT // CT)
        for i in range(MAXT):
            group = lists[s * MAXT + i] // CT - ids[0] * (RT // CT)
            for g in range(RT // CT):
                where[g] = jnp.where((i < order) & (group == g), i, where[g])
        for g in range(RT // CT):
            piece = panels[k, jnp.maximum(where[g], 0)]
            mine[k, g] = jnp.where(where[g] >= 0, piece, jnp.zeros_like(piece))
    copies = [pltpu.make_async_copy(mine, out.at[c], sems.at[c]) for c in range(COLS)]
    for copy in copies:
        copy.start()
    for copy in copies:
        copy.wait()


def hp_kernel(table, a0, a1, a2, a3, b0, b1, b2, b3, panels, hp, pt, wide):
    table = Table(table)
    ids, lists, orders, pattern = table.ids, table.lists, table.orders, table.pattern
    half = RT * TILE // 2
    c0 = ids[1] // 4
    c1 = ids[1] % 4
    for k in range(4):
        for m in range(4):
            first = (c0 + k) % 4 * 4 + (c1 + m) % 4
            second = (c0 + m) % 4 * 4 + (c1 + k) % 4
            for part, ref, col in ((0, (a0, a1, a2, a3)[k], first), (1, (b0, b1, b2, b3)[k], second)):
                for i in range(RT // 2):
                    for j in range(CT):
                        a = part * (RT // 2) + i
                        b = col * CT + j
                        tile = ref[m, pl.ds(i * TILE, TILE), pl.ds(j * TILE, TILE)]
                        live = kept(pattern, ids[0] * RT + a, b)
                        wide[
                            pl.ds(a * TILE, TILE), pl.ds(pl.multiple_of(b * TILE, TILE), TILE)
                        ] = jnp.where(live, tile, jnp.zeros_like(tile))
    pt[...] = jnp.zeros_like(pt)
    for k in range(ROWS):
        s = ids[1] * ROWS + k
        for i in range(MAXT):

            @pl.when(i < orders[s])
            def _():
                where = pl.multiple_of(lists[s * MAXT + i] * TILE, TILE)
                pt[pl.ds(k * CW, CW), pl.ds(where, TILE)] = panels[k, i]

    hp[...] = lax.dot_general(
        wide[...], pt[...], (((1,), (1,)), ((), ())), preferred_element_type=F32
    ).astype(BF16)


def final_kernel(table, present, pieces, *refs):
    blocks = refs[:8]
    density, php, pt, hp = refs[8:]
    ids = Table(table).ids
    join_rows(ids, blocks, hp)

    def place(c, _):
        for r in range(ROWS):
            s = c * ROWS + r
            here = pl.ds(pl.multiple_of(s * CW, CW), CW)
            for g in range(RT // CT):
                piece = pieces[c, r, g]
                for a in range(g * CT, g * CT + CT):
                    live = present[s * RT + a] > 0
                    pt[here, pl.ds(a * TILE, TILE)] = jnp.where(live, piece, jnp.zeros_like(piece))
        return 0

    lax.fori_loop(0, COLS, place, 0)
    php[...] = lax.dot_general(
        pt[...], hp[...], (((0,), (0,)), ((), ())), preferred_element_type=F32
    )
    mine = pt[pl.ds(pl.multiple_of(ids[1] * WIDTH, WIDTH), WIDTH), :]
    density[...] = mine.T


def from_ring(x, axis):
    return [x] + [lax.ppermute(x, axis, [((i + k) % 4, i) for i in range(4)]) for k in range(1, 4)]


def swapped(x):
    return lax.ppermute(x, "core", [(0, 1), (1, 0)])


SMEM = pl.BlockSpec(memory_space=pltpu.SMEM)
LOCAL = pl.BlockSpec(memory_space=pltpu.VMEM)
FAR = pl.BlockSpec(memory_space=pl.ANY)


def call(kernel, outs, scratch, small, large, specs=LOCAL, space=pltpu.VMEM):
    return pl.pallas_call(
        kernel,
        out_shape=outs,
        in_specs=[SMEM] * len(small) + [LOCAL if space is pltpu.VMEM else FAR] * len(large),
        out_specs=specs,
        scratch_shapes=scratch,
        compiler_params=pltpu.CompilerParams(vmem_limit_bytes=24 << 20),
    )(*small, *[pltpu.with_memory_space_constraint(x, space) for x in large])


def call_solve(table, shift, tiles, first):
    return call(
        solve_kernel,
        pltpu.VMEM((MAXT, CW, TILE), BF16),
        [pltpu.VMEM((N, N), BF16)] * 3,
        (table, shift),
        (tiles, first),
    )


def steps(hamiltonian, pattern, tile_lists, orders, shift):
    row = lax.axis_index(ROW)
    col = lax.axis_index(COL)
    ids = jnp.stack([row, col]).astype(jnp.int32)
    table = jnp.concatenate([tile_lists.reshape(-1), orders, pattern.reshape(-1), ids])
    half = RT * TILE // 2
    top, bottom = hamiltonian[:half], hamiltonian[half:]
    strip = from_ring(hamiltonian, "z")
    across = from_ring(bottom, "c0")
    ahead = from_ring(top, "c1")
    strip = strip + [swapped(x) for x in strip]
    packed, first = call(
        pack_kernel,
        (pltpu.HBM((COLS, 4, TILE, TILE), BF16), pltpu.HBM((MAXT, TILE, TILE), BF16)),
        [pltpu.VMEM((NB * TILE, WIDTH), BF16), pltpu.SemaphoreType.DMA((COLS + 2, 4))],
        (table,),
        (top, bottom, *strip[1:]),
        (FAR, FAR),
    )
    tiles = lax.all_to_all(packed, COL, 0, 0, tiled=True)
    across = from_ring(jnp.stack(across), "c1")
    ahead = from_ring(jnp.stack(ahead), "c0")
    panel = call_solve(table, shift, tiles, first)
    panels = lax.all_gather(panel, ROW, axis=0, tiled=False)
    spread = call(
        spread_kernel,
        pltpu.HBM((COLS, ROWS, RT // CT, CW, TILE), BF16),
        [pltpu.VMEM((ROWS, RT // CT, CW, TILE), BF16), pltpu.SemaphoreType.DMA((COLS,))],
        (table,),
        (panels,),
        FAR,
    )
    arrived = lax.all_to_all(spread, COL, 0, 0, tiled=True)
    hp = call(
        hp_kernel,
        pltpu.VMEM((RT * TILE, WIDTH), BF16),
        [pltpu.VMEM((WIDTH, NB * TILE), BF16), pltpu.VMEM((RT * TILE, NB * TILE), BF16)],
        (table,),
        (*ahead, *across, panels),
    )
    ours = from_ring(hp, "z")
    theirs = [swapped(x) for x in ours]
    own = row * RT + jnp.arange(RT, dtype=jnp.int32)
    live = jnp.arange(MAXT, dtype=jnp.int32)[None, :] < orders[:, None]
    present = jnp.any((tile_lists[:, None, :] == own[None, :, None]) & live[:, None, :], axis=2)
    density, php = call(
        final_kernel,
        (
            jax.ShapeDtypeStruct((RT * TILE, WIDTH), BF16),
            jax.ShapeDtypeStruct((RT * TILE, WIDTH), F32),
        ),
        [pltpu.VMEM((NB * TILE, RT * TILE), BF16), pltpu.VMEM((NB * TILE, WIDTH), BF16)],
        (table, present.astype(jnp.int32).reshape(-1)),
        (arrived, *ours, *theirs),
        (LOCAL, LOCAL),
    )
    return density, php


def solution(mesh):
    fine = Mesh(mesh.devices.reshape(4, 2, 4, 4), ("z", "core", "c0", "c1"))
    split = P(ROW, COL)
    return jax.shard_map(
        steps,
        mesh=fine,
        in_specs=(split, P(), P(), P(), P()),
        out_specs=(split, split),
        check_vma=False,
    )
```
